32 devices in a mesh: aux: 4 (over y, x), pair: 8 (over z, core).
Axes of the slice: x: 2, y: 2, z: 4, core: 2. Of those that a mesh axis runs over, the one named last changes fastest.
Arguments:
- m_panels: bfloat16 [40000, 8192], P('aux', 'pair'), may hold values from -6 to 6
- lower_cols: bfloat16 [2, 512, 40000], P(None, 'pair', 'aux'), may hold values from -0.2 to 0.2, as said below
- diag_inverses: float32 [2, 512, 512], replicated, may hold values from -0.2 to 2, as said below
Outputs:
- remainder: bfloat16 [40000, 8192], P('aux', 'pair')
- solved: bfloat16 [2, 512, 8192], P(None, None, 'pair')
The draws below stay inside these ranges and needn't reach their ends.
Inputs may be any that keep to these rules, and one draw needn't show every extreme that they name: lower_cols[k] is zero in the pivot rows of panels 0 to k (the factor is lower triangular and its diagonal blocks are given by their inverses). Each diag_inverses[k] is lower triangular.
All inputs are finite; a program needn't handle non-finite values.
Results may differ from the reference program's by a relative error of at most 0.0047.
Values may be sent and summed in bfloat16 or wider, within the bound.
A program may use at most 192 MiB of HBM per device.

```python
import jax
import jax.numpy as jnp
from jax import lax

NAUX = 40000
NB = 512
PANELS = 2
PAIR_DEV = 1024
AUX_ROWS = 10000
NPAIR = 8192
N_PAIR = 8


def draw_lower_cols(key, part):
    scale = 1.0 / (PANELS * NB) ** 0.5
    values = jnp.clip(jax.random.normal(key, (PANELS, NB, NAUX), jnp.float32), -6.0, 6.0)
    rows = jnp.arange(NAUX, dtype=jnp.int32)
    block = rows // AUX_ROWS
    within = rows % AUX_ROWS
    panel = jnp.arange(PANELS, dtype=jnp.int32)[:, None]
    keep = jnp.logical_not(jnp.logical_and(within[None, :] < NB, block[None, :] <= panel))
    values = jnp.clip(values * scale, -0.199, 0.199) * keep.astype(jnp.float32)[:, None, :]
    return values.astype(jnp.bfloat16)


def draw_diag_inverses(key, part):
    first = jax.random.fold_in(key, 11)
    second = jax.random.fold_in(key, 12)
    lower = jnp.clip(jax.random.normal(first, (PANELS, NB, NB), jnp.float32), -6.0, 6.0)
    lower = jnp.clip(lower * (0.7 / NB ** 0.5), -0.199, 0.199) * jnp.tril(jnp.ones((NB, NB), jnp.float32), -1)[None]
    diagonal = jnp.exp(jax.random.uniform(second, (PANELS, NB), jnp.float32, -0.69, 0.69))
    return lower + diagonal[:, :, None] * jnp.eye(NB, dtype=jnp.float32)[None]


def levels(own_key, extent, split, smallest, high):
    factor_of, own = 1.0, jax.random.fold_in(own_key, 6)
    for dim, parts in split:
        heights = jnp.exp(jax.random.uniform(jax.random.fold_in(own, dim), (parts,), jnp.float32, smallest / len(split), high / len(split)))
        factor_of = factor_of * jnp.repeat(heights, extent[dim] // parts).reshape([-1 if axis == dim else 1 for axis in range(len(extent))])
    return factor_of


def scatter_about(rng, extent, spread, most, split=(), held_as=jnp.bfloat16):
    drawn = spread * jax.random.normal(rng, extent, jnp.float32)
    if split:
        drawn = drawn * levels(rng, extent, split, -0.22, 0.18)
    return jnp.clip(drawn, -most, most).astype(held_as)


def setup_inputs(seed: int = 0) -> dict:
    key_list = jax.random.split(jax.random.key(seed), 4)
    m_panels = scatter_about(key_list[0], (NAUX, NPAIR), 1.0, 6.0, ((0, 4), (1, 8)))
    lower_cols = draw_lower_cols(jax.random.fold_in(key_list[3], 71), 0)
    diag_inverses = draw_diag_inverses(jax.random.fold_in(key_list[3], 71), 0)
    return dict(m_panels=m_panels, lower_cols=lower_cols, diag_inverses=diag_inverses)


def one_group(block_cols, lower_cols, diag_inverses):
    work = block_cols.astype(jnp.float32)
    results = []
    for panel in range(PANELS):
        first = panel * AUX_ROWS
        pivot = work[first:first + NB]
        solved_rows = jnp.dot(diag_inverses[panel], pivot, precision=lax.Precision.HIGHEST, preferred_element_type=jnp.float32).astype(jnp.bfloat16)
        work = work - jnp.dot(lower_cols[panel].T, solved_rows, preferred_element_type=jnp.float32)
        results.append(solved_rows)
    return work.astype(jnp.bfloat16), jnp.stack(results)


def reference(m_panels, lower_cols, diag_inverses):
    groups = m_panels.reshape(NAUX, N_PAIR, PAIR_DEV).transpose(1, 0, 2)
    remains, solves = lax.map(lambda cols: one_group(cols, lower_cols, diag_inverses), groups)
    remainder = remains.transpose(1, 0, 2).reshape(NAUX, N_PAIR * PAIR_DEV)
    solved = solves.transpose(1, 2, 0, 3).reshape(PANELS, NB, N_PAIR * PAIR_DEV)
    return remainder, solved
```

```python
import functools

import jax
import jax.numpy as jnp
from jax import lax
from jax.experimental import pallas as pl
from jax.experimental.pallas import tpu as pltpu
from jax.sharding import PartitionSpec as P

CHUNK = 1024
TILE = 256
LANES = 128
CORES = 2
WINDOW = 2
CONTRACT = (((0,), (0,)), ((), ()))
MESH = pl.DeviceIdType.MESH


def gather_kernel(aux, chips, chunk, m_hbm, l_hbm, d_hbm, mbuf, sbuf, ltail,
                  lbuf, ebuf, dbuf, load_sem, ring_sem, swap_sem, left_sem, right_sem, part_sem,
                  srecv_sem, ssend_sem):
    rows, columns = m_hbm.shape
    panels, width = d_hbm.shape[:2]
    whole = lbuf.shape[-1]
    mains = whole // chunk
    tail = ltail.shape[-1]
    pieces = mains + 1
    a = lax.axis_index("aux")
    me = lax.axis_index("pair")
    z, c = me // CORES, lax.rem(me, CORES)
    to_left = {"pair": lax.rem(z + chips - 1, chips) * CORES + c}
    to_right = {"pair": lax.rem(z + 1, chips) * CORES + c}
    partner = {"pair": z * CORES + 1 - c}

    def local(src, dst, i):
        return pltpu.make_async_copy(src, dst, load_sem.at[i])

    head_load = local(l_hbm.at[:, :, pl.ds(0, chunk)], lbuf.at[me, :, :, pl.ds(0, chunk)], 0)
    body_load = local(l_hbm.at[:, :, pl.ds(chunk, whole - chunk)],
                      lbuf.at[me, :, :, pl.ds(chunk, whole - chunk)], 1)
    tail_load = local(l_hbm.at[:, :, pl.ds(whole, rows - whole)], ebuf, 2)
    pivot_load = local(m_hbm.at[pl.ds(0, width)], mbuf.at[pl.ds(0, width)], 3)
    rest_load = local(m_hbm.at[pl.ds(width, rows - width)],
                      mbuf.at[pl.ds(width, rows - width)], 4)
    inverse_load = local(d_hbm, dbuf, 5)
    head_load.start()

    barrier = pltpu.get_barrier_semaphore()
    for peer in (to_left, to_right, partner):
        pl.semaphore_signal(barrier, inc=1, device_id=peer, device_id_type=MESH)
    for step in range(1, aux):
        peer = {"aux": lax.rem(a + step, aux)}
        pl.semaphore_signal(barrier, inc=1, device_id=peer, device_id_type=MESH)
    body_load.start()
    tail_load.start()
    pivot_load.start()
    inverse_load.start()
    pl.semaphore_wait(barrier, 2 + aux)
    head_load.wait()

    def piece(block, j, size):
        if size == chunk:
            return lbuf.at[block, :, :, pl.ds(pl.multiple_of(j * chunk, LANES), chunk)]
        return ltail.at[block]

    def ring(zb, j, size, send, peer):
        ref = piece(zb * CORES + c, j, size)
        return pltpu.make_async_remote_copy(
            src_ref=ref, dst_ref=ref, send_sem=send.at[zb, j], recv_sem=ring_sem.at[zb, j],
            device_id=peer, device_id_type=MESH)

    def swap(zb, j, size, core):
        ref = piece(zb * CORES + core, j, size)
        return pltpu.make_async_remote_copy(
            src_ref=ref, dst_ref=ref, send_sem=part_sem.at[zb, j], recv_sem=swap_sem.at[zb, j],
            device_id=partner, device_id_type=MESH)

    def sized(j, act):
        @pl.when(jnp.logical_and(j >= 0, j < mains))
        def _():
            act(j, chunk)

        @pl.when(j == mains)
        def _():
            act(mains, tail)

    def send(zb, j, size, leftward, rightward):
        @pl.when(jnp.logical_and(leftward, z > 0))
        def _():
            ring(zb, j, size, left_sem, to_left).start()

        @pl.when(jnp.logical_and(rightward, z < chips - 1))
        def _():
            ring(zb, j, size, right_sem, to_right).start()

        swap(zb, j, size, c).start()

    def sent(zb, j, size, leftward, rightward):
        @pl.when(jnp.logical_and(leftward, z > 0))
        def _():
            ring(zb, j, size, left_sem, to_left).wait_send()

        @pl.when(jnp.logical_and(rightward, z < chips - 1))
        def _():
            ring(zb, j, size, right_sem, to_right).wait_send()

        swap(zb, j, size, c).wait_send()

    def own(j, size):
        send(z, j, size, True, True)

    def own_sent(j, size):
        sent(z, j, size, True, True)

    def pass_on(step, j, size):
        @pl.when(z + step < chips)
        def _():
            ring(z + step, j, size, left_sem, to_left).wait_recv()
            send(z + step, j, size, True, False)

        @pl.when(z >= step)
        def _():
            ring(z - step, j, size, right_sem, to_right).wait_recv()
            send(z - step, j, size, False, True)

    def passed(step, j, size):
        @pl.when(z + step < chips)
        def _():
            sent(z + step, j, size, True, False)

        @pl.when(z >= step)
        def _():
            sent(z - step, j, size, False, True)

    def complete(j, size):
        for zb in range(chips):
            swap(zb, j, size, 1 - c).wait_recv()

    def solve(panel):
        def columns_of(i, _):
            cols = pl.ds(pl.multiple_of(i * TILE, TILE), TILE)
            pivot = mbuf[pl.ds(0, width), cols].astype(jnp.float32)
            for before in range(panel):
                factor = lbuf[:, before, :, pl.ds(0, width)].reshape(-1, width)
                pivot = pivot - lax.dot_general(
                    factor, sbuf[before, :, cols], CONTRACT, preferred_element_type=jnp.float32)
            sbuf[panel, :, cols] = jnp.dot(
                dbuf[panel], pivot, precision=lax.Precision.HIGHEST,
                preferred_element_type=jnp.float32).astype(jnp.bfloat16)
            return 0

        lax.fori_loop(0, columns // TILE, columns_of, 0)

    def spread(panel, step):
        return pltpu.make_async_remote_copy(
            src_ref=sbuf.at[panel], dst_ref=sbuf.at[panel],
            send_sem=ssend_sem.at[panel, step], recv_sem=srecv_sem.at[panel],
            device_id={"aux": lax.rem(a + step, aux)}, device_id_type=MESH)

    def settle(panel):
        solve(panel)
        for step in range(1, aux):
            spread(panel, step).start()

    def update(j, _):
        def tile(i, _):
            here = pl.ds(pl.multiple_of(i * TILE, TILE), TILE)
            product = sum(
                lax.dot_general(
                    lbuf[:, panel, :, here].reshape(-1, TILE), sbuf[panel], CONTRACT,
                    preferred_element_type=jnp.float32)
                for panel in range(panels))
            mbuf[here] = (mbuf[here].astype(jnp.float32) - product).astype(jnp.bfloat16)
            return 0

        tiles = chunk // TILE
        lax.fori_loop(j * tiles, (j + 1) * tiles, tile, 0)
        return 0

    last = pieces + chips
    first = min(chips + panels + 1, last - 1 - (mains + 1) // 2)

    def done_by(t):
        ready = jnp.minimum(t - chips + 1, 2 * (t - first + 1))
        return jnp.clip(jnp.where(t == last - 1, mains, ready), 0, mains)

    def tick(t, _):
        sized(t - WINDOW, own_sent)
        sized(t, own)
        sized(t - chips, complete)

        for panel in range(1, panels):
            @pl.when(jnp.logical_and(t == chips - 1 + panel, a == panel))
            def _(panel=panel):
                for before in range(panel):
                    spread(before, 1).wait_recv()
                settle(panel)

        @pl.when(t == first)
        def _():
            rest_load.wait()
            for panel in range(panels):
                @pl.when(jnp.logical_and(a != panel, jnp.logical_or(a < panel, a >= panels)))
                def _(panel=panel):
                    spread(panel, 1).wait_recv()

        lax.fori_loop(done_by(t - 1), done_by(t), update, 0)
        for step in range(1, chips):
            sized(t - WINDOW - step, functools.partial(passed, step))
            sized(t - step, functools.partial(pass_on, step))
        return 0

    own(jnp.int32(0), chunk)
    body_load.wait()
    tail_load.wait()
    rest_load.start()
    ltail[me, :, :, pl.ds(0, rows - whole)] = ebuf[...]
    own(jnp.int32(1), chunk)
    pivot_load.wait()
    inverse_load.wait()

    @pl.when(a == 0)
    def _():
        settle(0)

    for step in range(1, chips):
        sized(jnp.int32(1 - step), functools.partial(pass_on, step))
    lax.fori_loop(2, last, tick, 0)

    def drain(t, _):
        sized(t - WINDOW, own_sent)
        for step in range(1, chips):
            sized(t - WINDOW - step, functools.partial(passed, step))
        return 0

    lax.fori_loop(last, last + WINDOW, drain, 0)
    for panel in range(panels):
        @pl.when(a == panel)
        def _(panel=panel):
            for step in range(1, aux):
                spread(panel, step).wait_send()


def write_kernel(chunk, mbuf, sbuf, ltail, out_hbm, solved_hbm, tbuf, out_sem, tail_sem, s_sem):
    rows = mbuf.shape[0]
    panels = sbuf.shape[0]
    mains = out_sem.shape[0]
    whole = mains * chunk

    def main(j):
        here = pl.ds(pl.multiple_of(j * chunk, chunk), chunk)
        return pltpu.make_async_copy(mbuf.at[here], out_hbm.at[here], out_sem.at[j])

    lax.fori_loop(0, mains, lambda j, _: (main(j).start(), 0)[1], 0)
    solved = pltpu.make_async_copy(sbuf, solved_hbm, s_sem)
    solved.start()

    def product(here, size):
        return sum(
            lax.dot_general(
                ltail[:, panel, :, here].reshape(-1, size), sbuf[panel], CONTRACT,
                preferred_element_type=jnp.float32)
            for panel in range(panels))

    left = rows - whole
    full = left // TILE
    for i in range(full):
        here = pl.ds(i * TILE, TILE)
        total = mbuf[pl.ds(whole + i * TILE, TILE)].astype(jnp.float32) - product(here, TILE)
        tbuf[here] = total.astype(jnp.bfloat16)
    if left % TILE:
        here = pl.ds(full * TILE, left % TILE)
        size = min(-(-(left % TILE) // LANES) * LANES, ltail.shape[-1] - full * TILE)
        total = product(pl.ds(full * TILE, size), size)[:left % TILE]
        total = mbuf[pl.ds(whole + full * TILE, left % TILE)].astype(jnp.float32) - total
        tbuf[here] = total.astype(jnp.bfloat16)
    final = pltpu.make_async_copy(tbuf, out_hbm.at[pl.ds(whole, left)], tail_sem)
    lax.fori_loop(0, mains, lambda j, _: (main(j).wait(), 0)[1], 0)
    final.start()
    solved.wait()
    final.wait()


def shards(aux, pair, m_panels, lower_cols, diag_inverses):
    panels, width = diag_inverses.shape[:2]
    rows, columns = m_panels.shape
    part = lower_cols.shape[1]
    chips = pair // CORES
    padded = -(-rows // LANES) * LANES
    chunk = max(CHUNK, -(-width // TILE) * TILE)
    mains = (rows - 1) // chunk
    tail = padded - mains * chunk
    pieces = mains + 1
    anywhere = pl.BlockSpec(memory_space=pl.ANY)
    vmem = pl.BlockSpec(memory_space=pltpu.VMEM)
    dma = pltpu.SemaphoreType.DMA
    held, solved, ltail = pl.pallas_call(
        functools.partial(gather_kernel, aux, chips, chunk),
        in_specs=[anywhere, anywhere, anywhere],
        out_specs=[vmem, vmem, vmem],
        out_shape=[
            pltpu.VMEM((rows, columns), jnp.bfloat16),
            pltpu.VMEM((panels, width, columns), jnp.bfloat16),
            pltpu.VMEM((pair, panels, part, tail), jnp.bfloat16),
        ],
        scratch_shapes=[
            pltpu.VMEM((pair, panels, part, mains * chunk), jnp.bfloat16),
            pltpu.VMEM((panels, part, rows - mains * chunk), jnp.bfloat16),
            pltpu.VMEM((panels, width, width), jnp.float32),
            dma((6,)),
            dma((chips, pieces)),
            dma((chips, pieces)),
            dma((chips, pieces)),
            dma((chips, pieces)),
            dma((chips, pieces)),
            dma((panels,)),
            dma((panels, aux)),
        ],
        compiler_params=pltpu.CompilerParams(
            collective_id=0, has_side_effects=True, vmem_limit_bytes=36 * 1024 * 1024),
    )(m_panels, lower_cols, diag_inverses)
    return pl.pallas_call(
        functools.partial(write_kernel, chunk),
        in_specs=[vmem, vmem, vmem],
        out_specs=[anywhere, anywhere],
        out_shape=[
            jax.ShapeDtypeStruct((rows, columns), jnp.bfloat16),
            jax.ShapeDtypeStruct((panels, width, columns), jnp.bfloat16),
        ],
        scratch_shapes=[
            pltpu.VMEM((rows - mains * chunk, columns), jnp.bfloat16),
            dma((mains,)),
            dma,
            dma,
        ],
        compiler_params=pltpu.CompilerParams(vmem_limit_bytes=8 * 1024 * 1024),
    )(held, solved, ltail)


def solution(mesh):
    placed = (P("aux", "pair"), P(None, "pair", "aux"), P())
    return jax.shard_map(
        functools.partial(shards, mesh.shape["aux"], mesh.shape["pair"]),
        mesh=mesh,
        in_specs=placed,
        out_specs=(P("aux", "pair"), P(None, None, "pair")),
        check_vma=False,
    )
```

```python
import functools

import jax
import jax.numpy as jnp
from jax import lax
from jax.experimental import pallas as pl
from jax.experimental.pallas import tpu as pltpu
from jax.sharding import PartitionSpec as P

CHUNK = 1024
LATE = 1
TILE = 256
LANES = 128
SUBLANES = 16
CORES = 2
WINDOW = 2
CONTRACT = (((0,), (0,)), ((), ()))
MESH = pl.DeviceIdType.MESH


def packing(left, groups):
    ragged = left % LANES
    return left // LANES, ragged, LANES // ragged if ragged else groups


def tail_rows(panels, part, left):
    groups = panels * part // SUBLANES
    tiles, ragged, fit = packing(left, groups)
    return panels * tiles * part + (-(-groups // fit) * SUBLANES if ragged else 0)


def late_pieces(chunk, panels, part, left):
    tiles = left // LANES
    cuts = {0, max(0, tiles - TILE // LANES)}
    for k in range(1, LATE + 1):
        cuts.add(min(k * (chunk // LANES), tiles))
    cuts = sorted(cuts)
    starts = [cut * panels * part for cut in cuts]
    ends = starts[1:] + [tail_rows(panels, part, left)]
    return [(start, end - start) for start, end in zip(starts, ends) if end > start]


def pack(ebuf, ltail, me):
    panels, part, left = ebuf.shape
    groups = panels * part // SUBLANES
    tiles, ragged, fit = packing(left, groups)
    for panel in range(panels):
        for i in range(tiles):
            at = (i * panels + panel) * part
            ltail[me, pl.ds(at, part)] = ebuf[panel, :, pl.ds(i * LANES, LANES)]
    if not ragged:
        return
    base = panels * tiles * part
    end = ebuf[:, :, pl.ds(tiles * LANES, ragged)].reshape(groups, SUBLANES, ragged)
    row = lax.broadcasted_iota(jnp.int32, (ragged, LANES), 0)
    lane = lax.broadcasted_iota(jnp.int32, (ragged, LANES), 1)
    for slot in range(-(-groups // fit)):
        total = jnp.zeros((SUBLANES, LANES), jnp.float32)
        for g in range(slot * fit, min(groups, (slot + 1) * fit)):
            place = (lane == row + (g - slot * fit) * ragged).astype(jnp.bfloat16)
            total = total + jnp.dot(end[g], place, preferred_element_type=jnp.float32)
        ltail[me, pl.ds(base + slot * SUBLANES, SUBLANES)] = total.astype(jnp.bfloat16)


def gather_kernel(aux, chips, chunk, m_hbm, l_hbm, d_hbm, mbuf, sbuf, ltail,
                  lbuf, ebuf, dbuf, load_sem, ring_sem, swap_sem, left_sem, right_sem, part_sem,
                  srecv_sem, ssend_sem):
    rows, columns = m_hbm.shape
    panels, width = d_hbm.shape[:2]
    whole = lbuf.shape[-1]
    mains = whole // chunk
    left = rows - whole
    late = late_pieces(chunk, panels, l_hbm.shape[1], left)
    pieces = mains + len(late)
    a = lax.axis_index("aux")
    me = lax.axis_index("pair")
    z, c = me // CORES, lax.rem(me, CORES)
    to_left = {"pair": lax.rem(z + chips - 1, chips) * CORES + c}
    to_right = {"pair": lax.rem(z + 1, chips) * CORES + c}
    partner = {"pair": z * CORES + 1 - c}

    def local(src, dst, i):
        return pltpu.make_async_copy(src, dst, load_sem.at[i])

    head_load = local(l_hbm.at[:, :, pl.ds(0, chunk)], lbuf.at[me, :, :, pl.ds(0, chunk)], 0)
    body_load = local(l_hbm.at[:, :, pl.ds(chunk, whole - chunk)],
                      lbuf.at[me, :, :, pl.ds(chunk, whole - chunk)], 1)
    tail_load = local(l_hbm.at[:, :, pl.ds(whole, left)], ebuf, 2)
    pivot_load = local(m_hbm.at[pl.ds(0, width)], mbuf.at[pl.ds(0, width)], 3)
    rest_load = local(m_hbm.at[pl.ds(width, rows - width)],
                      mbuf.at[pl.ds(width, rows - width)], 4)
    inverse_load = local(d_hbm, dbuf, 5)
    head_load.start()

    barrier = pltpu.get_barrier_semaphore()
    for peer in (to_left, to_right, partner):
        pl.semaphore_signal(barrier, inc=1, device_id=peer, device_id_type=MESH)
    for step in range(1, aux):
        peer = {"aux": lax.rem(a + step, aux)}
        pl.semaphore_signal(barrier, inc=1, device_id=peer, device_id_type=MESH)
    body_load.start()
    tail_load.start()
    pivot_load.start()
    inverse_load.start()
    pl.semaphore_wait(barrier, 2 + aux)
    head_load.wait()

    def piece(block, j, size):
        if size == chunk:
            return lbuf.at[block, :, :, pl.ds(pl.multiple_of(j * chunk, LANES), chunk)]
        return ltail.at[block, pl.ds(*size)]

    def ring(zb, j, size, send, peer):
        ref = piece(zb * CORES + c, j, size)
        return pltpu.make_async_remote_copy(
            src_ref=ref, dst_ref=ref, send_sem=send.at[zb, j], recv_sem=ring_sem.at[zb, j],
            device_id=peer, device_id_type=MESH)

    def swap(zb, j, size, core):
        ref = piece(zb * CORES + core, j, size)
        return pltpu.make_async_remote_copy(
            src_ref=ref, dst_ref=ref, send_sem=part_sem.at[zb, j], recv_sem=swap_sem.at[zb, j],
            device_id=partner, device_id_type=MESH)

    def sized(j, act):
        @pl.when(jnp.logical_and(j >= 0, j < mains))
        def _():
            act(j, chunk)

        for k, span in enumerate(late):
            @pl.when(j == mains + k)
            def _(k=k, span=span):
                act(mains + k, span)

    def send(zb, j, size, leftward, rightward):
        @pl.when(jnp.logical_and(leftward, z > 0))
        def _():
            ring(zb, j, size, left_sem, to_left).start()

        @pl.when(jnp.logical_and(rightward, z < chips - 1))
        def _():
            ring(zb, j, size, right_sem, to_right).start()

        swap(zb, j, size, c).start()

    def sent(zb, j, size, leftward, rightward):
        @pl.when(jnp.logical_and(leftward, z > 0))
        def _():
            ring(zb, j, size, left_sem, to_left).wait_send()

        @pl.when(jnp.logical_and(rightward, z < chips - 1))
        def _():
            ring(zb, j, size, right_sem, to_right).wait_send()

        swap(zb, j, size, c).wait_send()

    def own(j, size):
        send(z, j, size, True, True)

    def own_sent(j, size):
        sent(z, j, size, True, True)

    def pass_on(step, j, size):
        @pl.when(z + step < chips)
        def _():
            ring(z + step, j, size, left_sem, to_left).wait_recv()
            send(z + step, j, size, True, False)

        @pl.when(z >= step)
        def _():
            ring(z - step, j, size, right_sem, to_right).wait_recv()
            send(z - step, j, size, False, True)

    def passed(step, j, size):
        @pl.when(z + step < chips)
        def _():
            sent(z + step, j, size, True, False)

        @pl.when(z >= step)
        def _():
            sent(z - step, j, size, False, True)

    def complete(j, size):
        for zb in range(chips):
            swap(zb, j, size, 1 - c).wait_recv()

    def solve(panel):
        def columns_of(i, _):
            cols = pl.ds(pl.multiple_of(i * TILE, TILE), TILE)
            pivot = mbuf[pl.ds(0, width), cols].astype(jnp.float32)
            for before in range(panel):
                factor = lbuf[:, before, :, pl.ds(0, width)].reshape(-1, width)
                pivot = pivot - lax.dot_general(
                    factor, sbuf[before, :, cols], CONTRACT, preferred_element_type=jnp.float32)
            sbuf[panel, :, cols] = jnp.dot(
                dbuf[panel], pivot, precision=lax.Precision.HIGHEST,
                preferred_element_type=jnp.float32).astype(jnp.bfloat16)
            return 0

        lax.fori_loop(0, columns // TILE, columns_of, 0)

    def spread(panel, step):
        return pltpu.make_async_remote_copy(
            src_ref=sbuf.at[panel], dst_ref=sbuf.at[panel],
            send_sem=ssend_sem.at[panel, step], recv_sem=srecv_sem.at[panel],
            device_id={"aux": lax.rem(a + step, aux)}, device_id_type=MESH)

    def settle(panel):
        solve(panel)
        for step in range(1, aux):
            spread(panel, step).start()

    def update(j, _):
        def tile(i, _):
            here = pl.ds(pl.multiple_of(i * TILE, TILE), TILE)
            product = sum(
                lax.dot_general(
                    lbuf[:, panel, :, here].reshape(-1, TILE), sbuf[panel], CONTRACT,
                    preferred_element_type=jnp.float32)
                for panel in range(panels))
            mbuf[here] = (mbuf[here].astype(jnp.float32) - product).astype(jnp.bfloat16)
            return 0

        tiles = chunk // TILE
        lax.fori_loop(j * tiles, (j + 1) * tiles, tile, 0)
        return 0

    last = pieces + chips
    first = min(chips + panels + 1, last - 1 - (mains + 1) // 2)

    def done_by(t):
        ready = jnp.minimum(t - chips + 1, 2 * (t - first + 1))
        return jnp.clip(jnp.where(t == last - 1, mains, ready), 0, mains)

    def tick(t, _):
        sized(t - WINDOW, own_sent)
        sized(t, own)
        sized(t - chips, complete)

        @pl.when(t == first)
        def _():
            rest_load.wait()
            for panel in range(panels):
                @pl.when(jnp.logical_and(a != panel, jnp.logical_or(a < panel, a >= panels)))
                def _(panel=panel):
                    spread(panel, 1).wait_recv()

        lax.fori_loop(done_by(t - 1), done_by(t), update, 0)
        for step in range(1, chips):
            sized(t - WINDOW - step, functools.partial(passed, step))
            sized(t - step, functools.partial(pass_on, step))
        for panel in range(panels):
            @pl.when(jnp.logical_and(t == (chips - 1 + panel if panel else 2), a == panel))
            def _(panel=panel):
                for before in range(panel):
                    spread(before, 1).wait_recv()
                settle(panel)
        return 0

    own(jnp.int32(0), chunk)
    body_load.wait()
    tail_load.wait()
    rest_load.start()
    pack(ebuf, ltail, me)
    own(jnp.int32(1), chunk)
    for step in range(1, chips):
        sized(jnp.int32(1 - step), functools.partial(pass_on, step))
    pivot_load.wait()
    inverse_load.wait()
    lax.fori_loop(2, last, tick, 0)

    def drain(t, _):
        sized(t - WINDOW, own_sent)
        for step in range(1, chips):
            sized(t - WINDOW - step, functools.partial(passed, step))
        return 0

    lax.fori_loop(last, last + WINDOW, drain, 0)
    for panel in range(panels):
        @pl.when(a == panel)
        def _(panel=panel):
            for step in range(1, aux):
                spread(panel, step).wait_send()


def write_kernel(chunk, mbuf, sbuf, ltail, out_hbm, solved_hbm, tbuf, out_sem, tail_sem, s_sem):
    rows = mbuf.shape[0]
    panels, width = sbuf.shape[:2]
    pair = ltail.shape[0]
    mains = out_sem.shape[0]
    whole = mains * chunk

    def main(j):
        here = pl.ds(pl.multiple_of(j * chunk, chunk), chunk)
        return pltpu.make_async_copy(mbuf.at[here], out_hbm.at[here], out_sem.at[j])

    lax.fori_loop(0, mains, lambda j, _: (main(j).start(), 0)[1], 0)
    solved = pltpu.make_async_copy(sbuf, solved_hbm, s_sem)
    solved.start()

    left = rows - whole
    part = width // pair
    groups = panels * part // SUBLANES
    tiles, ragged, fit = packing(left, groups)

    def store(at, total):
        here = pl.ds(at, total.shape[0])
        held = mbuf[pl.ds(whole + at, total.shape[0])].astype(jnp.float32)
        tbuf[here] = (held - total).astype(jnp.bfloat16)

    def lanes_of(panel, i):
        return ltail[:, pl.ds((i * panels + panel) * part, part)].reshape(width, LANES)

    for i in range(0, tiles, TILE // LANES):
        both = range(i, min(tiles, i + TILE // LANES))
        store(i * LANES, sum(
            lax.dot_general(
                jnp.concatenate([lanes_of(panel, i) for i in both], axis=1), sbuf[panel], CONTRACT,
                preferred_element_type=jnp.float32)
            for panel in range(panels)))
    if ragged:
        base = panels * tiles * part
        total = 0.0
        for g in range(groups):
            slot, off = g // fit, g % fit * ragged
            panel, at = g * SUBLANES // part, g * SUBLANES % part
            packed = ltail[:, pl.ds(base + slot * SUBLANES, SUBLANES)].reshape(-1, LANES)
            solved_rows = sbuf[panel].reshape(pair, part, -1)[:, at:at + SUBLANES]
            total = total + lax.dot_general(
                packed, solved_rows.reshape(pair * SUBLANES, -1), CONTRACT,
                preferred_element_type=jnp.float32)[off:off + ragged]
        store(tiles * LANES, total)
    final = pltpu.make_async_copy(tbuf, out_hbm.at[pl.ds(whole, left)], tail_sem)
    early = mains // 2
    lax.fori_loop(0, early, lambda j, _: (main(j).wait(), 0)[1], 0)
    final.start()
    lax.fori_loop(early, mains, lambda j, _: (main(j).wait(), 0)[1], 0)
    solved.wait()
    final.wait()


def shards(aux, pair, m_panels, lower_cols, diag_inverses):
    panels, width = diag_inverses.shape[:2]
    rows, columns = m_panels.shape
    part = lower_cols.shape[1]
    chips = pair // CORES
    chunk = max(CHUNK, -(-width // TILE) * TILE)
    mains = (rows - 1) // chunk - LATE
    left = rows - mains * chunk
    pieces = mains + len(late_pieces(chunk, panels, part, left))
    anywhere = pl.BlockSpec(memory_space=pl.ANY)
    vmem = pl.BlockSpec(memory_space=pltpu.VMEM)
    dma = pltpu.SemaphoreType.DMA
    held, solved, ltail = pl.pallas_call(
        functools.partial(gather_kernel, aux, chips, chunk),
        in_specs=[anywhere, anywhere, anywhere],
        out_specs=[vmem, vmem, vmem],
        out_shape=[
            pltpu.VMEM((rows, columns), jnp.bfloat16),
            pltpu.VMEM((panels, width, columns), jnp.bfloat16),
            pltpu.VMEM((pair, tail_rows(panels, part, left), LANES), jnp.bfloat16),
        ],
        scratch_shapes=[
            pltpu.VMEM((pair, panels, part, mains * chunk), jnp.bfloat16),
            pltpu.VMEM((panels, part, left), jnp.bfloat16),
            pltpu.VMEM((panels, width, width), jnp.float32),
            dma((6,)),
            dma((chips, pieces)),
            dma((chips, pieces)),
            dma((chips, pieces)),
            dma((chips, pieces)),
            dma((chips, pieces)),
            dma((panels,)),
            dma((panels, aux)),
        ],
        compiler_params=pltpu.CompilerParams(
            collective_id=0, has_side_effects=True, vmem_limit_bytes=36 * 1024 * 1024),
    )(m_panels, lower_cols, diag_inverses)
    return pl.pallas_call(
        functools.partial(write_kernel, chunk),
        in_specs=[vmem, vmem, vmem],
        out_specs=[anywhere, anywhere],
        out_shape=[
            jax.ShapeDtypeStruct((rows, columns), jnp.bfloat16),
            jax.ShapeDtypeStruct((panels, width, columns), jnp.bfloat16),
        ],
        scratch_shapes=[
            pltpu.VMEM((left, columns), jnp.bfloat16),
            dma((mains,)),
            dma,
            dma,
        ],
        compiler_params=pltpu.CompilerParams(vmem_limit_bytes=8 * 1024 * 1024),
    )(held, solved, ltail)


def solution(mesh):
    placed = (P("aux", "pair"), P(None, "pair", "aux"), P())
    return jax.shard_map(
        functools.partial(shards, mesh.shape["aux"], mesh.shape["pair"]),
        mesh=mesh,
        in_specs=placed,
        out_specs=(P("aux", "pair"), P(None, None, "pair")),
        check_vma=False,
    )
```

```python
import functools

import jax
import jax.numpy as jnp
from jax import lax
from jax.experimental import pallas as pl
from jax.experimental.pallas import tpu as pltpu
from jax.sharding import PartitionSpec as P

CHUNK = 1024
LATE = 1
TILE = 256
LANES = 128
SUBLANES = 16
CORES = 2
WINDOW = 2
CONTRACT = (((0,), (0,)), ((), ()))
MESH = pl.DeviceIdType.MESH


def packing(left, groups):
    ragged = left % LANES
    return left // LANES, ragged, LANES // ragged if ragged else groups


def tail_rows(panels, part, left):
    groups = panels * part // SUBLANES
    tiles, ragged, fit = packing(left, groups)
    return panels * tiles * part + (-(-groups // fit) * SUBLANES if ragged else 0)


def late_pieces(chunk, panels, part, left):
    tiles = left // LANES
    cuts = {0, max(0, tiles - TILE // LANES)}
    for k in range(1, LATE + 1):
        cuts.add(min(k * (chunk // LANES), tiles))
    cuts = sorted(cuts)
    starts = [cut * panels * part for cut in cuts]
    ends = starts[1:] + [tail_rows(panels, part, left)]
    return [(start, end - start) for start, end in zip(starts, ends) if end > start]


def pack(ebuf, ltail, me):
    panels, part, left = ebuf.shape
    groups = panels * part // SUBLANES
    tiles, ragged, fit = packing(left, groups)
    for panel in range(panels):
        for i in range(tiles):
            at = (i * panels + panel) * part
            ltail[me, pl.ds(at, part)] = ebuf[panel, :, pl.ds(i * LANES, LANES)]
    if not ragged:
        return
    base = panels * tiles * part
    end = ebuf[:, :, pl.ds(tiles * LANES, ragged)].reshape(groups, SUBLANES, ragged)
    row = lax.broadcasted_iota(jnp.int32, (ragged, LANES), 0)
    lane = lax.broadcasted_iota(jnp.int32, (ragged, LANES), 1)
    for slot in range(-(-groups // fit)):
        total = jnp.zeros((SUBLANES, LANES), jnp.float32)
        for g in range(slot * fit, min(groups, (slot + 1) * fit)):
            place = (lane == row + (g - slot * fit) * ragged).astype(jnp.bfloat16)
            total = total + jnp.dot(end[g], place, preferred_element_type=jnp.float32)
        ltail[me, pl.ds(base + slot * SUBLANES, SUBLANES)] = total.astype(jnp.bfloat16)


def gather_kernel(aux, chips, chunk, m_hbm, l_hbm, d_hbm, mbuf, sbuf, ltail,
                  lbuf, ebuf, dbuf, load_sem, ring_sem, swap_sem, left_sem, right_sem, part_sem,
                  srecv_sem, ssend_sem):
    rows, columns = m_hbm.shape
    panels, width = d_hbm.shape[:2]
    whole = lbuf.shape[-1]
    mains = whole // chunk
    left = rows - whole
    late = late_pieces(chunk, panels, l_hbm.shape[1], left)
    pieces = mains + len(late)
    a = lax.axis_index("aux")
    me = lax.axis_index("pair")
    z, c = me // CORES, lax.rem(me, CORES)
    to_left = {"pair": lax.rem(z + chips - 1, chips) * CORES + c}
    to_right = {"pair": lax.rem(z + 1, chips) * CORES + c}
    partner = {"pair": z * CORES + 1 - c}

    def local(src, dst, i):
        return pltpu.make_async_copy(src, dst, load_sem.at[i])

    head_load = local(l_hbm.at[:, :, pl.ds(0, chunk)], lbuf.at[me, :, :, pl.ds(0, chunk)], 0)
    body_load = local(l_hbm.at[:, :, pl.ds(chunk, whole - chunk)],
                      lbuf.at[me, :, :, pl.ds(chunk, whole - chunk)], 1)
    tail_load = local(l_hbm.at[:, :, pl.ds(whole, left)], ebuf, 2)
    pivot_load = local(m_hbm.at[pl.ds(0, width)], mbuf.at[pl.ds(0, width)], 3)
    rest_load = local(m_hbm.at[pl.ds(width, rows - width)],
                      mbuf.at[pl.ds(width, rows - width)], 4)
    inverse_load = local(d_hbm, dbuf, 5)
    head_load.start()

    barrier = pltpu.get_barrier_semaphore()
    for peer in (to_left, to_right, partner):
        pl.semaphore_signal(barrier, inc=1, device_id=peer, device_id_type=MESH)
    for step in range(1, aux):
        peer = {"aux": lax.rem(a + step, aux)}
        pl.semaphore_signal(barrier, inc=1, device_id=peer, device_id_type=MESH)
    body_load.start()
    tail_load.start()
    pivot_load.start()
    inverse_load.start()
    pl.semaphore_wait(barrier, 2 + aux)
    head_load.wait()

    def piece(block, j, size):
        if size == chunk:
            return lbuf.at[block, :, :, pl.ds(pl.multiple_of(j * chunk, LANES), chunk)]
        if size is None:
            return lbuf.at[block, :, :, pl.ds(width, chunk - width)]
        return ltail.at[block, pl.ds(*size)]

    def ring(zb, j, size, send, peer):
        ref = piece(zb * CORES + c, j, size)
        return pltpu.make_async_remote_copy(
            src_ref=ref, dst_ref=ref, send_sem=send.at[zb, j], recv_sem=ring_sem.at[zb, j],
            device_id=peer, device_id_type=MESH)

    def swap(zb, j, size, core):
        ref = piece(zb * CORES + core, j, size)
        return pltpu.make_async_remote_copy(
            src_ref=ref, dst_ref=ref, send_sem=part_sem.at[zb, j], recv_sem=swap_sem.at[zb, j],
            device_id=partner, device_id_type=MESH)

    def sized(j, act):
        bare = jnp.logical_and(j == 0, a == 0)

        @pl.when(jnp.logical_and(jnp.logical_not(bare), jnp.logical_and(j >= 0, j < mains)))
        def _():
            act(j, chunk)

        @pl.when(bare)
        def _():
            act(0, None)

        for k, span in enumerate(late):
            @pl.when(j == mains + k)
            def _(k=k, span=span):
                act(mains + k, span)

    def send(zb, j, size, leftward, rightward):
        @pl.when(jnp.logical_and(leftward, z > 0))
        def _():
            ring(zb, j, size, left_sem, to_left).start()

        @pl.when(jnp.logical_and(rightward, z < chips - 1))
        def _():
            ring(zb, j, size, right_sem, to_right).start()

        swap(zb, j, size, c).start()

    def sent(zb, j, size, leftward, rightward):
        @pl.when(jnp.logical_and(leftward, z > 0))
        def _():
            ring(zb, j, size, left_sem, to_left).wait_send()

        @pl.when(jnp.logical_and(rightward, z < chips - 1))
        def _():
            ring(zb, j, size, right_sem, to_right).wait_send()

        swap(zb, j, size, c).wait_send()

    def own(j, size):
        send(z, j, size, True, True)

    def own_sent(j, size):
        sent(z, j, size, True, True)

    def pass_on(step, j, size):
        @pl.when(z + step < chips)
        def _():
            ring(z + step, j, size, left_sem, to_left).wait_recv()
            send(z + step, j, size, True, False)

        @pl.when(z >= step)
        def _():
            ring(z - step, j, size, right_sem, to_right).wait_recv()
            send(z - step, j, size, False, True)

    def passed(step, j, size):
        @pl.when(z + step < chips)
        def _():
            sent(z + step, j, size, True, False)

        @pl.when(z >= step)
        def _():
            sent(z - step, j, size, False, True)

    def complete(j, size):
        for zb in range(chips):
            swap(zb, j, size, 1 - c).wait_recv()

    def solve(panel):
        def columns_of(i, _):
            cols = pl.ds(pl.multiple_of(i * TILE, TILE), TILE)
            pivot = mbuf[pl.ds(0, width), cols].astype(jnp.float32)
            for before in range(panel):
                factor = lbuf[:, before, :, pl.ds(0, width)].reshape(-1, width)
                pivot = pivot - lax.dot_general(
                    factor, sbuf[before, :, cols], CONTRACT, preferred_element_type=jnp.float32)
            sbuf[panel, :, cols] = jnp.dot(
                dbuf[panel], pivot, precision=lax.Precision.HIGHEST,
                preferred_element_type=jnp.float32).astype(jnp.bfloat16)
            return 0

        lax.fori_loop(0, columns // TILE, columns_of, 0)

    def spread(panel, step):
        return pltpu.make_async_remote_copy(
            src_ref=sbuf.at[panel], dst_ref=sbuf.at[panel],
            send_sem=ssend_sem.at[panel, step], recv_sem=srecv_sem.at[panel],
            device_id={"aux": lax.rem(a + step, aux)}, device_id_type=MESH)

    def settle(panel):
        solve(panel)
        for step in range(1, aux):
            spread(panel, step).start()

    def update(j, _):
        def tile(i, _):
            here = pl.ds(pl.multiple_of(i * TILE, TILE), TILE)
            product = sum(
                lax.dot_general(
                    lbuf[:, panel, :, here].reshape(-1, TILE), sbuf[panel], CONTRACT,
                    preferred_element_type=jnp.float32)
                for panel in range(panels))
            mbuf[here] = (mbuf[here].astype(jnp.float32) - product).astype(jnp.bfloat16)
            return 0

        tiles = chunk // TILE
        lax.fori_loop(j * tiles, (j + 1) * tiles, tile, 0)
        return 0

    last = pieces + chips
    first = min(chips + panels + 1, last - 1 - (mains + 1) // 2)

    def done_by(t):
        ready = jnp.minimum(t - chips + 1, 2 * (t - first + 1))
        return jnp.clip(jnp.where(t == last - 1, mains, ready), 0, mains)

    def tick(t, _):
        sized(t - WINDOW, own_sent)
        sized(t, own)
        sized(t - chips, complete)

        @pl.when(t == first)
        def _():
            rest_load.wait()
            for panel in range(panels):
                @pl.when(jnp.logical_and(a != panel, jnp.logical_or(a < panel, a >= panels)))
                def _(panel=panel):
                    spread(panel, 1).wait_recv()

        lax.fori_loop(done_by(t - 1), done_by(t), update, 0)
        for step in range(1, chips):
            sized(t - WINDOW - step, functools.partial(passed, step))
            sized(t - step, functools.partial(pass_on, step))
        for panel in range(panels):
            @pl.when(jnp.logical_and(t == (chips - 1 + panel if panel else 2), a == panel))
            def _(panel=panel):
                for before in range(panel):
                    spread(before, 1).wait_recv()
                settle(panel)
        return 0

    sized(jnp.int32(0), own)
    body_load.wait()
    tail_load.wait()
    rest_load.start()
    pack(ebuf, ltail, me)
    own(jnp.int32(1), chunk)

    @pl.when(a == 0)
    def _():
        lbuf[:, :, :, pl.ds(0, width)] = jnp.zeros(lbuf.shape[:3] + (width,), jnp.bfloat16)

    for step in range(1, chips):
        sized(jnp.int32(1 - step), functools.partial(pass_on, step))
    pivot_load.wait()
    inverse_load.wait()
    lax.fori_loop(2, last, tick, 0)

    def drain(t, _):
        sized(t - WINDOW, own_sent)
        for step in range(1, chips):
            sized(t - WINDOW - step, functools.partial(passed, step))
        return 0

    lax.fori_loop(last, last + WINDOW, drain, 0)
    for panel in range(panels):
        @pl.when(a == panel)
        def _(panel=panel):
            for step in range(1, aux):
                spread(panel, step).wait_send()


def write_kernel(chunk, mbuf, sbuf, ltail, out_hbm, solved_hbm, tbuf, out_sem, tail_sem, s_sem):
    rows = mbuf.shape[0]
    panels, width = sbuf.shape[:2]
    pair = ltail.shape[0]
    mains = out_sem.shape[0]
    whole = mains * chunk

    def main(j):
        here = pl.ds(pl.multiple_of(j * chunk, chunk), chunk)
        return pltpu.make_async_copy(mbuf.at[here], out_hbm.at[here], out_sem.at[j])

    lax.fori_loop(0, mains, lambda j, _: (main(j).start(), 0)[1], 0)
    solved = pltpu.make_async_copy(sbuf, solved_hbm, s_sem)
    solved.start()

    left = rows - whole
    part = width // pair
    groups = panels * part // SUBLANES
    tiles, ragged, fit = packing(left, groups)

    def store(at, total):
        here = pl.ds(at, total.shape[0])
        held = mbuf[pl.ds(whole + at, total.shape[0])].astype(jnp.float32)
        tbuf[here] = (held - total).astype(jnp.bfloat16)

    def lanes_of(panel, i):
        return ltail[:, pl.ds((i * panels + panel) * part, part)].reshape(width, LANES)

    for i in range(0, tiles, TILE // LANES):
        both = range(i, min(tiles, i + TILE // LANES))
        store(i * LANES, sum(
            lax.dot_general(
                jnp.concatenate([lanes_of(panel, i) for i in both], axis=1), sbuf[panel], CONTRACT,
                preferred_element_type=jnp.float32)
            for panel in range(panels)))
    if ragged:
        base = panels * tiles * part
        total = 0.0
        for g in range(groups):
            slot, off = g // fit, g % fit * ragged
            panel, at = g * SUBLANES // part, g * SUBLANES % part
            packed = ltail[:, pl.ds(base + slot * SUBLANES, SUBLANES)].reshape(-1, LANES)
            solved_rows = sbuf[panel].reshape(pair, part, -1)[:, at:at + SUBLANES]
            total = total + lax.dot_general(
                packed, solved_rows.reshape(pair * SUBLANES, -1), CONTRACT,
                preferred_element_type=jnp.float32)[off:off + ragged]
        store(tiles * LANES, total)
    final = pltpu.make_async_copy(tbuf, out_hbm.at[pl.ds(whole, left)], tail_sem)
    early = mains // 2
    lax.fori_loop(0, early, lambda j, _: (main(j).wait(), 0)[1], 0)
    final.start()
    lax.fori_loop(early, mains, lambda j, _: (main(j).wait(), 0)[1], 0)
    solved.wait()
    final.wait()


def shards(aux, pair, m_panels, lower_cols, diag_inverses):
    panels, width = diag_inverses.shape[:2]
    rows, columns = m_panels.shape
    part = lower_cols.shape[1]
    chips = pair // CORES
    chunk = max(CHUNK, (width // TILE + 1) * TILE)
    mains = (rows - 1) // chunk - LATE
    left = rows - mains * chunk
    pieces = mains + len(late_pieces(chunk, panels, part, left))
    anywhere = pl.BlockSpec(memory_space=pl.ANY)
    vmem = pl.BlockSpec(memory_space=pltpu.VMEM)
    dma = pltpu.SemaphoreType.DMA
    held, solved, ltail = pl.pallas_call(
        functools.partial(gather_kernel, aux, chips, chunk),
        in_specs=[anywhere, anywhere, anywhere],
        out_specs=[vmem, vmem, vmem],
        out_shape=[
            pltpu.VMEM((rows, columns), jnp.bfloat16),
            pltpu.VMEM((panels, width, columns), jnp.bfloat16),
            pltpu.VMEM((pair, tail_rows(panels, part, left), LANES), jnp.bfloat16),
        ],
        scratch_shapes=[
            pltpu.VMEM((pair, panels, part, mains * chunk), jnp.bfloat16),
            pltpu.VMEM((panels, part, left), jnp.bfloat16),
            pltpu.VMEM((panels, width, width), jnp.float32),
            dma((6,)),
            dma((chips, pieces)),
            dma((chips, pieces)),
            dma((chips, pieces)),
            dma((chips, pieces)),
            dma((chips, pieces)),
            dma((panels,)),
            dma((panels, aux)),
        ],
        compiler_params=pltpu.CompilerParams(
            collective_id=0, has_side_effects=True, vmem_limit_bytes=36 * 1024 * 1024),
    )(m_panels, lower_cols, diag_inverses)
    return pl.pallas_call(
        functools.partial(write_kernel, chunk),
        in_specs=[vmem, vmem, vmem],
        out_specs=[anywhere, anywhere],
        out_shape=[
            jax.ShapeDtypeStruct((rows, columns), jnp.bfloat16),
            jax.ShapeDtypeStruct((panels, width, columns), jnp.bfloat16),
        ],
        scratch_shapes=[
            pltpu.VMEM((left, columns), jnp.bfloat16),
            dma((mains,)),
            dma,
            dma,
        ],
        compiler_params=pltpu.CompilerParams(vmem_limit_bytes=8 * 1024 * 1024),
    )(held, solved, ltail)


def solution(mesh):
    placed = (P("aux", "pair"), P(None, "pair", "aux"), P())
    return jax.shard_map(
        functools.partial(shards, mesh.shape["aux"], mesh.shape["pair"]),
        mesh=mesh,
        in_specs=placed,
        out_specs=(P("aux", "pair"), P(None, None, "pair")),
        check_vma=False,
    )
```

```python
import functools

import jax
import jax.numpy as jnp
from jax import lax
from jax.experimental import pallas as pl
from jax.experimental.pallas import tpu as pltpu
from jax.sharding import PartitionSpec as P

CHUNK = 1024
LATE = 1
TILE = 256
LANES = 128
SUBLANES = 16
CORES = 2
CUT = 1
HOPS = (2, 5, 6)
WINDOW = 2
CONTRACT = (((0,), (0,)), ((), ()))
MESH = pl.DeviceIdType.MESH


def packing(left, groups):
    ragged = left % LANES
    return left // LANES, ragged, LANES // ragged if ragged else groups


def tail_rows(panels, part, left):
    groups = panels * part // SUBLANES
    tiles, ragged, fit = packing(left, groups)
    return panels * tiles * part + (-(-groups // fit) * SUBLANES if ragged else 0)


def late_pieces(chunk, panels, part, left):
    tiles = left // LANES
    cuts = {0, max(0, tiles - TILE // LANES)}
    for k in range(1, LATE + 1):
        cuts.add(min(k * (chunk // LANES), tiles))
    cuts = sorted(cuts)
    starts = [cut * panels * part for cut in cuts]
    ends = starts[1:] + [tail_rows(panels, part, left)]
    return [(start, end - start) for start, end in zip(starts, ends) if end > start]


def pack(ebuf, ltail, me):
    panels, part, left = ebuf.shape
    groups = panels * part // SUBLANES
    tiles, ragged, fit = packing(left, groups)
    for panel in range(panels):
        for i in range(tiles):
            at = (i * panels + panel) * part
            ltail[me, pl.ds(at, part)] = ebuf[panel, :, pl.ds(i * LANES, LANES)]
    if not ragged:
        return
    base = panels * tiles * part
    end = ebuf[:, :, pl.ds(tiles * LANES, ragged)].reshape(groups, SUBLANES, ragged)
    row = lax.broadcasted_iota(jnp.int32, (ragged, LANES), 0)
    lane = lax.broadcasted_iota(jnp.int32, (ragged, LANES), 1)
    for slot in range(-(-groups // fit)):
        total = jnp.zeros((SUBLANES, LANES), jnp.float32)
        for g in range(slot * fit, min(groups, (slot + 1) * fit)):
            place = (lane == row + (g - slot * fit) * ragged).astype(jnp.bfloat16)
            total = total + jnp.dot(end[g], place, preferred_element_type=jnp.float32)
        ltail[me, pl.ds(base + slot * SUBLANES, SUBLANES)] = total.astype(jnp.bfloat16)


def gather_kernel(aux, chips, chunk, cut_at, m_hbm, l_hbm, d_hbm, mbuf, sbuf, ltail,
                  lbuf, ebuf, dbuf, rbuf, load_sem, ring_sem, swap_sem, left_sem, right_sem, part_sem,
                  srecv_sem, ssend_sem, hop_sem, relay_sem):
    rows, columns = m_hbm.shape
    panels, width = d_hbm.shape[:2]
    whole = lbuf.shape[-1]
    mains = whole // chunk
    left = rows - whole
    late = late_pieces(chunk, panels, l_hbm.shape[1], left)
    pieces = mains + len(late)
    edge_at = pieces + 1
    detours = rbuf.shape[0]
    a = lax.axis_index("aux")
    me = lax.axis_index("pair")
    z, c = me // CORES, lax.rem(me, CORES)
    to_left = {"pair": lax.rem(z + chips - 1, chips) * CORES + c}
    to_right = {"pair": lax.rem(z + 1, chips) * CORES + c}
    partner = {"pair": z * CORES + 1 - c}

    def local(src, dst, i):
        return pltpu.make_async_copy(src, dst, load_sem.at[i])

    head_load = local(l_hbm.at[:, :, pl.ds(0, chunk)], lbuf.at[me, :, :, pl.ds(0, chunk)], 0)
    body_load = local(l_hbm.at[:, :, pl.ds(chunk, whole - chunk)],
                      lbuf.at[me, :, :, pl.ds(chunk, whole - chunk)], 1)
    tail_load = local(l_hbm.at[:, :, pl.ds(whole, left)], ebuf, 2)
    pivot_load = local(m_hbm.at[pl.ds(0, width)], mbuf.at[pl.ds(0, width)], 3)
    rest_load = local(m_hbm.at[pl.ds(width, rows - width)],
                      mbuf.at[pl.ds(width, rows - width)], 4)
    inverse_load = local(d_hbm, dbuf, 5)
    head_load.start()

    barrier = pltpu.get_barrier_semaphore()
    for peer in (to_left, to_right, partner):
        pl.semaphore_signal(barrier, inc=1, device_id=peer, device_id_type=MESH)
    for step in range(1, aux):
        peer = {"aux": lax.rem(a + step, aux)}
        pl.semaphore_signal(barrier, inc=1, device_id=peer, device_id_type=MESH)
    body_load.start()
    tail_load.start()
    pivot_load.start()
    inverse_load.start()
    pl.semaphore_wait(barrier, 2 + aux)
    head_load.wait()

    def piece(block, j, kind):
        name, *span = kind
        if name == "late":
            return ltail.at[block, pl.ds(*span)]
        if name == "head":
            return lbuf.at[block, pl.ds(0, *span), :, pl.ds(0, width)]
        if name == "bare":
            return lbuf.at[block, :, :, pl.ds(width, chunk - width)]
        if name == "edge":
            return lbuf.at[block, :, :, pl.ds((cut_at + 1) * chunk - LANES, LANES)]
        if name == "cut":
            return lbuf.at[block, :, :, pl.ds(cut_at * chunk, chunk - LANES)]
        return lbuf.at[block, :, :, pl.ds(pl.multiple_of(j * chunk, LANES), chunk)]

    def ring(zb, j, size, send, peer):
        ref = piece(zb * CORES + c, j, size)
        return pltpu.make_async_remote_copy(
            src_ref=ref, dst_ref=ref, send_sem=send.at[zb, j], recv_sem=ring_sem.at[zb, j],
            device_id=peer, device_id_type=MESH)

    def swap(zb, j, size, core):
        ref = piece(zb * CORES + core, j, size)
        return pltpu.make_async_remote_copy(
            src_ref=ref, dst_ref=ref, send_sem=part_sem.at[zb, j], recv_sem=swap_sem.at[zb, j],
            device_id=partner, device_id_type=MESH)

    def sized(j, act):
        whole_piece = jnp.logical_or(j > 0, a >= panels)
        whole_piece = jnp.logical_and(whole_piece, jnp.logical_and(j >= 0, j < mains))
        whole_piece = jnp.logical_and(whole_piece, j != cut_at)

        @pl.when(whole_piece)
        def _():
            act(j, ("main",))

        for block in range(panels):
            @pl.when(jnp.logical_and(j == 0, a == block))
            def _(block=block):
                act(0, ("bare",))
                if block:
                    act(pieces, ("head", block))

        @pl.when(j == cut_at)
        def _():
            act(edge_at, ("edge",))
            act(cut_at, ("cut",))

        for k, span in enumerate(late):
            @pl.when(j == mains + k)
            def _(k=k, span=span):
                act(mains + k, ("late", *span))

    detoured = jnp.logical_and(a >= panels, a < panels + detours)
    lane = jnp.clip(a - panels, 0, max(detours - 1, 0))

    def via(zb, send):
        return pltpu.make_async_remote_copy(
            src_ref=piece(zb * CORES + c, edge_at, ("edge",)), dst_ref=rbuf.at[lane, zb],
            send_sem=send.at[zb, edge_at], recv_sem=hop_sem.at[0, lane, zb],
            device_id={"aux": 0}, device_id_type=MESH)

    def along(d, zb, peer):
        return pltpu.make_async_remote_copy(
            src_ref=rbuf.at[d, zb], dst_ref=rbuf.at[d, zb],
            send_sem=relay_sem.at[d, zb], recv_sem=hop_sem.at[1, d, zb],
            device_id=peer, device_id_type=MESH)

    def back(d, zb):
        return pltpu.make_async_remote_copy(
            src_ref=rbuf.at[d, zb], dst_ref=piece(zb * CORES + c, edge_at, ("edge",)),
            send_sem=relay_sem.at[d, zb], recv_sem=ring_sem.at[zb, edge_at],
            device_id={"aux": panels + d}, device_id_type=MESH)

    sides = ((0, 1, 1, to_left), (chips - 1, chips - 2, -1, to_right)) if detours else ()

    def hops(t):
        for end, near, sign, peer in sides:
            for d in range(detours):
                s = t - cut_at - HOPS[0]

                @pl.when(jnp.logical_and(a == 0, jnp.logical_and(
                    z == near, jnp.logical_and(s >= 0, s < chips - 1))))
                def _(s=s, d=d, near=near, sign=sign, peer=peer):
                    zb = near + sign * s
                    pltpu.make_async_remote_copy(
                        src_ref=rbuf.at[d, zb], dst_ref=rbuf.at[d, zb],
                        send_sem=relay_sem.at[d, zb], recv_sem=hop_sem.at[0, d, zb],
                        device_id=peer, device_id_type=MESH).wait_recv()
                    along(d, zb, peer).start()

                s = t - cut_at - HOPS[1]

                @pl.when(jnp.logical_and(a == 0, jnp.logical_and(
                    z == end, jnp.logical_and(s >= 0, s < chips - 1))))
                def _(s=s, d=d, near=near, sign=sign, peer=peer):
                    zb = near + sign * s
                    along(d, zb, peer).wait_recv()
                    back(d, zb).start()

            s = t - cut_at - HOPS[2]

            @pl.when(jnp.logical_and(detoured, jnp.logical_and(
                z == end, jnp.logical_and(s >= 0, s < chips - 1))))
            def _(s=s, near=near, sign=sign, peer=peer):
                zb = near + sign * s
                ring(zb, edge_at, ("edge",), left_sem, peer).wait_recv()
                swap(zb, edge_at, ("edge",), c).start()

    def hops_sent():
        for end, near, sign, peer in sides:
            def relayed(s, _, end=end, near=near, sign=sign, peer=peer):
                zb = near + sign * s
                for d in range(detours):
                    @pl.when(jnp.logical_and(a == 0, z == near))
                    def _(d=d):
                        along(d, zb, peer).wait_send()

                    @pl.when(jnp.logical_and(a == 0, z == end))
                    def _(d=d):
                        back(d, zb).wait_send()

                @pl.when(jnp.logical_and(detoured, z == end))
                def _():
                    swap(zb, edge_at, ("edge",), c).wait_send()
                return 0

            lax.fori_loop(0, chips - 1, relayed, 0)

    def leave(zb, j, size, leftward, rightward, act):
        goes_left = jnp.logical_and(leftward, z > 0)
        goes_right = jnp.logical_and(rightward, z < chips - 1)
        if size[0] == "edge" and detours:
            round_left = jnp.logical_and(goes_left, jnp.logical_and(detoured, z == 1))
            round_right = jnp.logical_and(goes_right, jnp.logical_and(detoured, z == chips - 2))
            goes_left = jnp.logical_and(goes_left, jnp.logical_not(round_left))
            goes_right = jnp.logical_and(goes_right, jnp.logical_not(round_right))

            @pl.when(round_left)
            def _():
                act(via(zb, left_sem))

            @pl.when(round_right)
            def _():
                act(via(zb, right_sem))

        @pl.when(goes_left)
        def _():
            act(ring(zb, j, size, left_sem, to_left))

        @pl.when(goes_right)
        def _():
            act(ring(zb, j, size, right_sem, to_right))

        act(swap(zb, j, size, c))

    def send(zb, j, size, leftward, rightward):
        leave(zb, j, size, leftward, rightward, lambda copy: copy.start())

    def sent(zb, j, size, leftward, rightward):
        leave(zb, j, size, leftward, rightward, lambda copy: copy.wait_send())

    def arrives(zb, size, end):
        here = jnp.logical_and(zb >= 0, zb < chips)
        if size[0] == "edge" and detours:
            here = jnp.logical_and(here, jnp.logical_not(jnp.logical_and(detoured, z == end)))
        return here

    def own(j, size):
        send(z, j, size, True, True)

    def own_sent(j, size):
        sent(z, j, size, True, True)

    def pass_on(step, j, size):
        @pl.when(arrives(z + step, size, 0))
        def _():
            ring(z + step, j, size, left_sem, to_left).wait_recv()
            send(z + step, j, size, True, False)

        @pl.when(arrives(z - step, size, chips - 1))
        def _():
            ring(z - step, j, size, right_sem, to_right).wait_recv()
            send(z - step, j, size, False, True)

    def passed(step, j, size):
        @pl.when(arrives(z + step, size, 0))
        def _():
            sent(z + step, j, size, True, False)

        @pl.when(arrives(z - step, size, chips - 1))
        def _():
            sent(z - step, j, size, False, True)

    def complete(j, size):
        if size[0] == "edge":
            return
        for zb in range(chips):
            swap(zb, j, size, 1 - c).wait_recv()

    def solve(panel):
        def columns_of(i, _):
            cols = pl.ds(pl.multiple_of(i * TILE, TILE), TILE)
            pivot = mbuf[pl.ds(0, width), cols].astype(jnp.float32)
            for before in range(panel):
                factor = lbuf[:, before, :, pl.ds(0, width)].reshape(-1, width)
                pivot = pivot - lax.dot_general(
                    factor, sbuf[before, :, cols], CONTRACT, preferred_element_type=jnp.float32)
            sbuf[panel, :, cols] = jnp.dot(
                dbuf[panel], pivot, precision=lax.Precision.HIGHEST,
                preferred_element_type=jnp.float32).astype(jnp.bfloat16)
            return 0

        lax.fori_loop(0, columns // TILE, columns_of, 0)

    def spread(panel, step):
        return pltpu.make_async_remote_copy(
            src_ref=sbuf.at[panel], dst_ref=sbuf.at[panel],
            send_sem=ssend_sem.at[panel, step], recv_sem=srecv_sem.at[panel],
            device_id={"aux": lax.rem(a + step, aux)}, device_id_type=MESH)

    def settle(panel):
        solve(panel)
        for step in range(1, aux):
            spread(panel, step).start()

    before_last = max(mains - 2, cut_at)

    def update(j, _):
        at = jnp.where(jnp.logical_or(j < cut_at, j == mains - 1), j, j + 1)
        at = jnp.where(j == before_last, cut_at, at)

        def tile(i, _):
            here = pl.ds(pl.multiple_of(i * TILE, TILE), TILE)
            product = sum(
                lax.dot_general(
                    lbuf[:, panel, :, here].reshape(-1, TILE), sbuf[panel], CONTRACT,
                    preferred_element_type=jnp.float32)
                for panel in range(panels))
            mbuf[here] = (mbuf[here].astype(jnp.float32) - product).astype(jnp.bfloat16)
            return 0

        tiles = chunk // TILE
        lax.fori_loop(at * tiles, (at + 1) * tiles, tile, 0)
        return 0

    edges_in = cut_at + HOPS[2] + chips - 1
    last = max(pieces + chips, edges_in + 1)
    first = min(chips + panels + 1, last - 1 - (mains + 1) // 2)

    def done_by(t):
        ready = jnp.where(t >= max(edges_in, before_last + chips), t - chips + 1,
                          jnp.minimum(t - chips, before_last))
        ready = jnp.minimum(ready, 2 * (t - first + 1))
        return jnp.clip(jnp.where(t == last - 1, mains, ready), 0, mains)

    def tick(t, _):
        sized(t - WINDOW, own_sent)
        sized(t, own)
        sized(t - chips, complete)

        @pl.when(t == edges_in)
        def _():
            for zb in range(chips):
                swap(zb, edge_at, ("edge",), 1 - c).wait_recv()

        @pl.when(t == first)
        def _():
            rest_load.wait()
            for panel in range(panels):
                @pl.when(jnp.logical_and(a != panel, jnp.logical_or(a < panel, a >= panels)))
                def _(panel=panel):
                    spread(panel, 1).wait_recv()

        lax.fori_loop(done_by(t - 1), done_by(t), update, 0)
        for step in range(1, chips):
            sized(t - WINDOW - step, functools.partial(passed, step))
            sized(t - step, functools.partial(pass_on, step))
        hops(t)
        for panel in range(panels):
            @pl.when(jnp.logical_and(t == (chips - 1 + panel if panel else 2), a == panel))
            def _(panel=panel):
                for before in range(panel):
                    spread(before, 1).wait_recv()
                settle(panel)
        return 0

    sized(jnp.int32(0), own)
    body_load.wait()
    tail_load.wait()
    rest_load.start()
    pack(ebuf, ltail, me)
    sized(jnp.int32(1), own)

    for block in range(panels):
        @pl.when(a == block)
        def _(block=block):
            shape = (lbuf.shape[0], panels - block, lbuf.shape[2], width)
            lbuf[:, pl.ds(block, panels - block), :, pl.ds(0, width)] = jnp.zeros(shape, jnp.bfloat16)

    for step in range(1, chips):
        sized(jnp.int32(1 - step), functools.partial(pass_on, step))
    pivot_load.wait()
    inverse_load.wait()
    lax.fori_loop(2, last, tick, 0)

    def drain(t, _):
        sized(t - WINDOW, own_sent)
        for step in range(1, chips):
            sized(t - WINDOW - step, functools.partial(passed, step))
        return 0

    lax.fori_loop(last, last + WINDOW, drain, 0)
    hops_sent()
    for panel in range(panels):
        @pl.when(a == panel)
        def _(panel=panel):
            for step in range(1, aux):
                spread(panel, step).wait_send()


def write_kernel(chunk, mbuf, sbuf, ltail, out_hbm, solved_hbm, tbuf, out_sem, tail_sem, s_sem):
    rows = mbuf.shape[0]
    panels, width = sbuf.shape[:2]
    pair = ltail.shape[0]
    mains = out_sem.shape[0]
    whole = mains * chunk

    def main(j):
        here = pl.ds(pl.multiple_of(j * chunk, chunk), chunk)
        return pltpu.make_async_copy(mbuf.at[here], out_hbm.at[here], out_sem.at[j])

    lax.fori_loop(0, mains, lambda j, _: (main(j).start(), 0)[1], 0)
    solved = pltpu.make_async_copy(sbuf, solved_hbm, s_sem)
    solved.start()

    left = rows - whole
    part = width // pair
    groups = panels * part // SUBLANES
    tiles, ragged, fit = packing(left, groups)

    def store(at, total):
        here = pl.ds(at, total.shape[0])
        held = mbuf[pl.ds(whole + at, total.shape[0])].astype(jnp.float32)
        tbuf[here] = (held - total).astype(jnp.bfloat16)

    def lanes_of(panel, i):
        return ltail[:, pl.ds((i * panels + panel) * part, part)].reshape(width, LANES)

    for i in range(0, tiles, TILE // LANES):
        both = range(i, min(tiles, i + TILE // LANES))
        store(i * LANES, sum(
            lax.dot_general(
                jnp.concatenate([lanes_of(panel, i) for i in both], axis=1), sbuf[panel], CONTRACT,
                preferred_element_type=jnp.float32)
            for panel in range(panels)))
    if ragged:
        base = panels * tiles * part
        total = 0.0
        for g in range(groups):
            slot, off = g // fit, g % fit * ragged
            panel, at = g * SUBLANES // part, g * SUBLANES % part
            packed = ltail[:, pl.ds(base + slot * SUBLANES, SUBLANES)].reshape(-1, LANES)
            solved_rows = sbuf[panel].reshape(pair, part, -1)[:, at:at + SUBLANES]
            total = total + lax.dot_general(
                packed, solved_rows.reshape(pair * SUBLANES, -1), CONTRACT,
                preferred_element_type=jnp.float32)[off:off + ragged]
        store(tiles * LANES, total)
    final = pltpu.make_async_copy(tbuf, out_hbm.at[pl.ds(whole, left)], tail_sem)
    early = mains // 2
    lax.fori_loop(0, early, lambda j, _: (main(j).wait(), 0)[1], 0)
    final.start()
    lax.fori_loop(early, mains, lambda j, _: (main(j).wait(), 0)[1], 0)
    solved.wait()
    final.wait()


def shards(aux, pair, m_panels, lower_cols, diag_inverses):
    panels, width = diag_inverses.shape[:2]
    rows, columns = m_panels.shape
    part = lower_cols.shape[1]
    chips = pair // CORES
    chunk = max(CHUNK, (width // TILE + 1) * TILE)
    mains = (rows - 1) // chunk - LATE
    left = rows - mains * chunk
    pieces = mains + len(late_pieces(chunk, panels, part, left))
    cut_at = min(CUT, mains - 1)
    detours = min(panels, aux - panels) if chips >= 4 else 0
    anywhere = pl.BlockSpec(memory_space=pl.ANY)
    vmem = pl.BlockSpec(memory_space=pltpu.VMEM)
    dma = pltpu.SemaphoreType.DMA
    held, solved, ltail = pl.pallas_call(
        functools.partial(gather_kernel, aux, chips, chunk, cut_at),
        in_specs=[anywhere, anywhere, anywhere],
        out_specs=[vmem, vmem, vmem],
        out_shape=[
            pltpu.VMEM((rows, columns), jnp.bfloat16),
            pltpu.VMEM((panels, width, columns), jnp.bfloat16),
            pltpu.VMEM((pair, tail_rows(panels, part, left), LANES), jnp.bfloat16),
        ],
        scratch_shapes=[
            pltpu.VMEM((pair, panels, part, mains * chunk), jnp.bfloat16),
            pltpu.VMEM((panels, part, left), jnp.bfloat16),
            pltpu.VMEM((panels, width, width), jnp.float32),
            pltpu.VMEM((detours, chips, panels, part, LANES), jnp.bfloat16),
            dma((6,)),
            dma((chips, pieces + 2)),
            dma((chips, pieces + 2)),
            dma((chips, pieces + 2)),
            dma((chips, pieces + 2)),
            dma((chips, pieces + 2)),
            dma((panels,)),
            dma((panels, aux)),
            dma((2, max(detours, 1), chips)),
            dma((max(detours, 1), chips)),
        ],
        compiler_params=pltpu.CompilerParams(
            collective_id=0, has_side_effects=True, vmem_limit_bytes=36 * 1024 * 1024),
    )(m_panels, lower_cols, diag_inverses)
    return pl.pallas_call(
        functools.partial(write_kernel, chunk),
        in_specs=[vmem, vmem, vmem],
        out_specs=[anywhere, anywhere],
        out_shape=[
            jax.ShapeDtypeStruct((rows, columns), jnp.bfloat16),
            jax.ShapeDtypeStruct((panels, width, columns), jnp.bfloat16),
        ],
        scratch_shapes=[
            pltpu.VMEM((left, columns), jnp.bfloat16),
            dma((mains,)),
            dma,
            dma,
        ],
        compiler_params=pltpu.CompilerParams(vmem_limit_bytes=8 * 1024 * 1024),
    )(held, solved, ltail)


def solution(mesh):
    placed = (P("aux", "pair"), P(None, "pair", "aux"), P())
    return jax.shard_map(
        functools.partial(shards, mesh.shape["aux"], mesh.shape["pair"]),
        mesh=mesh,
        in_specs=placed,
        out_specs=(P("aux", "pair"), P(None, None, "pair")),
        check_vma=False,
    )
```

```python
import functools

import jax
import jax.numpy as jnp
from jax import lax
from jax.experimental import pallas as pl
from jax.experimental.pallas import tpu as pltpu
from jax.sharding import PartitionSpec as P

CHUNK = 1024
LATE = 1
TILE = 256
LANES = 128
SUBLANES = 16
CORES = 2
CUT = 1
HOPS = (2, 5, 6)
ENDING = 4
WINDOW = 2
CONTRACT = (((0,), (0,)), ((), ()))
MESH = pl.DeviceIdType.MESH


def packing(left, groups):
    ragged = left % LANES
    return left // LANES, ragged, LANES // ragged if ragged else groups


def tail_rows(panels, part, left):
    groups = panels * part // SUBLANES
    tiles, ragged, fit = packing(left, groups)
    return panels * tiles * part + (-(-groups // fit) * SUBLANES if ragged else 0)


def late_pieces(chunk, panels, part, left):
    tiles = left // LANES
    cuts = {0, max(0, tiles - TILE // LANES)}
    for k in range(1, LATE + 1):
        cuts.add(min(k * (chunk // LANES), tiles))
    cuts = sorted(cuts)
    starts = [cut * panels * part for cut in cuts]
    ends = starts[1:] + [tail_rows(panels, part, left)]
    return [(start, end - start) for start, end in zip(starts, ends) if end > start]


def pack(ebuf, ltail, me):
    panels, part, left = ebuf.shape
    groups = panels * part // SUBLANES
    tiles, ragged, fit = packing(left, groups)
    for panel in range(panels):
        for i in range(tiles):
            at = (i * panels + panel) * part
            ltail[me, pl.ds(at, part)] = ebuf[panel, :, pl.ds(i * LANES, LANES)]
    if not ragged:
        return
    base = panels * tiles * part
    end = ebuf[:, :, pl.ds(tiles * LANES, ragged)].reshape(groups, SUBLANES, ragged)
    row = lax.broadcasted_iota(jnp.int32, (ragged, LANES), 0)
    lane = lax.broadcasted_iota(jnp.int32, (ragged, LANES), 1)
    for slot in range(-(-groups // fit)):
        total = jnp.zeros((SUBLANES, LANES), jnp.float32)
        for g in range(slot * fit, min(groups, (slot + 1) * fit)):
            place = (lane == row + (g - slot * fit) * ragged).astype(jnp.bfloat16)
            total = total + jnp.dot(end[g], place, preferred_element_type=jnp.float32)
        ltail[me, pl.ds(base + slot * SUBLANES, SUBLANES)] = total.astype(jnp.bfloat16)


def gather_kernel(aux, chips, chunk, cut_at, m_hbm, l_hbm, d_hbm, mbuf, sbuf, ltail,
                  lbuf, ebuf, dbuf, rbuf, load_sem, ring_sem, swap_sem, left_sem, right_sem, part_sem,
                  srecv_sem, ssend_sem, hop_sem, relay_sem):
    rows, columns = m_hbm.shape
    panels, width = d_hbm.shape[:2]
    whole = lbuf.shape[-1]
    mains = whole // chunk
    left = rows - whole
    late = late_pieces(chunk, panels, l_hbm.shape[1], left)
    pieces = mains + len(late)
    edge_at = pieces + 1
    detours = rbuf.shape[0]
    a = lax.axis_index("aux")
    me = lax.axis_index("pair")
    z, c = me // CORES, lax.rem(me, CORES)
    to_left = {"pair": lax.rem(z + chips - 1, chips) * CORES + c}
    to_right = {"pair": lax.rem(z + 1, chips) * CORES + c}
    partner = {"pair": z * CORES + 1 - c}

    def local(src, dst, i):
        return pltpu.make_async_copy(src, dst, load_sem.at[i])

    head_load = local(l_hbm.at[:, :, pl.ds(0, chunk)], lbuf.at[me, :, :, pl.ds(0, chunk)], 0)
    body_load = local(l_hbm.at[:, :, pl.ds(chunk, whole - chunk)],
                      lbuf.at[me, :, :, pl.ds(chunk, whole - chunk)], 1)
    tail_load = local(l_hbm.at[:, :, pl.ds(whole, left)], ebuf, 2)
    pivot_load = local(m_hbm.at[pl.ds(0, width)], mbuf.at[pl.ds(0, width)], 3)
    rest_load = local(m_hbm.at[pl.ds(width, rows - width)],
                      mbuf.at[pl.ds(width, rows - width)], 4)
    inverse_load = local(d_hbm, dbuf, 5)
    head_load.start()

    barrier = pltpu.get_barrier_semaphore()
    for peer in (to_left, to_right, partner):
        pl.semaphore_signal(barrier, inc=1, device_id=peer, device_id_type=MESH)
    for step in range(1, aux):
        peer = {"aux": lax.rem(a + step, aux)}
        pl.semaphore_signal(barrier, inc=1, device_id=peer, device_id_type=MESH)
    body_load.start()
    tail_load.start()
    pivot_load.start()
    inverse_load.start()
    pl.semaphore_wait(barrier, 2 + aux)
    head_load.wait()

    def piece(block, j, kind):
        name, *span = kind
        if name == "late":
            return ltail.at[block, pl.ds(*span)]
        if name == "head":
            return lbuf.at[block, pl.ds(0, *span), :, pl.ds(0, width)]
        if name == "bare":
            return lbuf.at[block, :, :, pl.ds(width, chunk - width)]
        if name == "edge":
            return lbuf.at[block, :, :, pl.ds((cut_at + 1) * chunk - LANES, LANES)]
        if name == "cut":
            return lbuf.at[block, :, :, pl.ds(cut_at * chunk, chunk - LANES)]
        at = j * chunk if isinstance(j, int) else pl.multiple_of(j * chunk, LANES)
        return lbuf.at[block, :, :, pl.ds(at, chunk)]

    def ring(zb, j, size, send, peer):
        ref = piece(zb * CORES + c, j, size)
        return pltpu.make_async_remote_copy(
            src_ref=ref, dst_ref=ref, send_sem=send.at[zb, j], recv_sem=ring_sem.at[zb, j],
            device_id=peer, device_id_type=MESH)

    def swap(zb, j, size, core):
        ref = piece(zb * CORES + core, j, size)
        return pltpu.make_async_remote_copy(
            src_ref=ref, dst_ref=ref, send_sem=part_sem.at[zb, j], recv_sem=swap_sem.at[zb, j],
            device_id=partner, device_id_type=MESH)

    def sized(j, act):
        if isinstance(j, int) and j > 0:
            if j == cut_at:
                act(edge_at, ("edge",))
                act(cut_at, ("cut",))
            elif j < mains:
                act(j, ("main",))
            elif j < pieces:
                act(j, ("late", *late[j - mains]))
            return
        if isinstance(j, int) and j < 0:
            return
        whole_piece = jnp.logical_or(j > 0, a >= panels)
        whole_piece = jnp.logical_and(whole_piece, jnp.logical_and(j >= 0, j < mains))
        whole_piece = jnp.logical_and(whole_piece, j != cut_at)

        @pl.when(whole_piece)
        def _():
            act(j, ("main",))

        for block in range(panels):
            @pl.when(jnp.logical_and(j == 0, a == block))
            def _(block=block):
                act(0, ("bare",))
                if block:
                    act(pieces, ("head", block))

        @pl.when(j == cut_at)
        def _():
            act(edge_at, ("edge",))
            act(cut_at, ("cut",))

        for k, span in enumerate(late):
            @pl.when(j == mains + k)
            def _(k=k, span=span):
                act(mains + k, ("late", *span))

    detoured = jnp.logical_and(a >= panels, a < panels + detours)
    lane = jnp.clip(a - panels, 0, max(detours - 1, 0))

    def via(zb, send):
        return pltpu.make_async_remote_copy(
            src_ref=piece(zb * CORES + c, edge_at, ("edge",)), dst_ref=rbuf.at[lane, zb],
            send_sem=send.at[zb, edge_at], recv_sem=hop_sem.at[0, lane, zb],
            device_id={"aux": 0}, device_id_type=MESH)

    def along(d, zb, peer):
        return pltpu.make_async_remote_copy(
            src_ref=rbuf.at[d, zb], dst_ref=rbuf.at[d, zb],
            send_sem=relay_sem.at[d, zb], recv_sem=hop_sem.at[1, d, zb],
            device_id=peer, device_id_type=MESH)

    def back(d, zb):
        return pltpu.make_async_remote_copy(
            src_ref=rbuf.at[d, zb], dst_ref=piece(zb * CORES + c, edge_at, ("edge",)),
            send_sem=relay_sem.at[d, zb], recv_sem=ring_sem.at[zb, edge_at],
            device_id={"aux": panels + d}, device_id_type=MESH)

    sides = ((0, 1, 1, to_left), (chips - 1, chips - 2, -1, to_right)) if detours else ()

    def hops(t):
        for end, near, sign, peer in sides:
            for d in range(detours):
                s = t - cut_at - HOPS[0]

                @pl.when(jnp.logical_and(a == 0, jnp.logical_and(
                    z == near, jnp.logical_and(s >= 0, s < chips - 1))))
                def _(s=s, d=d, near=near, sign=sign, peer=peer):
                    zb = near + sign * s
                    pltpu.make_async_remote_copy(
                        src_ref=rbuf.at[d, zb], dst_ref=rbuf.at[d, zb],
                        send_sem=relay_sem.at[d, zb], recv_sem=hop_sem.at[0, d, zb],
                        device_id=peer, device_id_type=MESH).wait_recv()
                    along(d, zb, peer).start()

                s = t - cut_at - HOPS[1]

                @pl.when(jnp.logical_and(a == 0, jnp.logical_and(
                    z == end, jnp.logical_and(s >= 0, s < chips - 1))))
                def _(s=s, d=d, near=near, sign=sign, peer=peer):
                    zb = near + sign * s
                    along(d, zb, peer).wait_recv()
                    back(d, zb).start()

            s = t - cut_at - HOPS[2]

            @pl.when(jnp.logical_and(detoured, jnp.logical_and(
                z == end, jnp.logical_and(s >= 0, s < chips - 1))))
            def _(s=s, near=near, sign=sign, peer=peer):
                zb = near + sign * s
                ring(zb, edge_at, ("edge",), left_sem, peer).wait_recv()
                swap(zb, edge_at, ("edge",), c).start()

    def hops_sent():
        for end, near, sign, peer in sides:
            def relayed(s, _, end=end, near=near, sign=sign, peer=peer):
                zb = near + sign * s
                for d in range(detours):
                    @pl.when(jnp.logical_and(a == 0, z == near))
                    def _(d=d):
                        along(d, zb, peer).wait_send()

                    @pl.when(jnp.logical_and(a == 0, z == end))
                    def _(d=d):
                        back(d, zb).wait_send()

                @pl.when(jnp.logical_and(detoured, z == end))
                def _():
                    swap(zb, edge_at, ("edge",), c).wait_send()
                return 0

            lax.fori_loop(0, chips - 1, relayed, 0)

    def leave(zb, j, size, leftward, rightward, act):
        goes_left = jnp.logical_and(leftward, z > 0)
        goes_right = jnp.logical_and(rightward, z < chips - 1)
        if size[0] == "edge" and detours:
            round_left = jnp.logical_and(goes_left, jnp.logical_and(detoured, z == 1))
            round_right = jnp.logical_and(goes_right, jnp.logical_and(detoured, z == chips - 2))
            goes_left = jnp.logical_and(goes_left, jnp.logical_not(round_left))
            goes_right = jnp.logical_and(goes_right, jnp.logical_not(round_right))

            @pl.when(round_left)
            def _():
                act(via(zb, left_sem))

            @pl.when(round_right)
            def _():
                act(via(zb, right_sem))

        @pl.when(goes_left)
        def _():
            act(ring(zb, j, size, left_sem, to_left))

        @pl.when(goes_right)
        def _():
            act(ring(zb, j, size, right_sem, to_right))

        act(swap(zb, j, size, c))

    def send(zb, j, size, leftward, rightward):
        leave(zb, j, size, leftward, rightward, lambda copy: copy.start())

    def sent(zb, j, size, leftward, rightward):
        leave(zb, j, size, leftward, rightward, lambda copy: copy.wait_send())

    def arrives(zb, size, end):
        here = jnp.logical_and(zb >= 0, zb < chips)
        if size[0] == "edge" and detours:
            here = jnp.logical_and(here, jnp.logical_not(jnp.logical_and(detoured, z == end)))
        return here

    def own(j, size):
        send(z, j, size, True, True)

    def own_sent(j, size):
        sent(z, j, size, True, True)

    def pass_on(step, j, size):
        @pl.when(arrives(z + step, size, 0))
        def _():
            ring(z + step, j, size, left_sem, to_left).wait_recv()
            send(z + step, j, size, True, False)

        @pl.when(arrives(z - step, size, chips - 1))
        def _():
            ring(z - step, j, size, right_sem, to_right).wait_recv()
            send(z - step, j, size, False, True)

    def passed(step, j, size):
        @pl.when(arrives(z + step, size, 0))
        def _():
            sent(z + step, j, size, True, False)

        @pl.when(arrives(z - step, size, chips - 1))
        def _():
            sent(z - step, j, size, False, True)

    def complete(j, size):
        if size[0] == "edge":
            return
        for zb in range(chips):
            swap(zb, j, size, 1 - c).wait_recv()

    def solve(panel):
        def columns_of(i, _):
            cols = pl.ds(pl.multiple_of(i * TILE, TILE), TILE)
            pivot = mbuf[pl.ds(0, width), cols].astype(jnp.float32)
            for before in range(panel):
                factor = lbuf[:, before, :, pl.ds(0, width)].reshape(-1, width)
                pivot = pivot - lax.dot_general(
                    factor, sbuf[before, :, cols], CONTRACT, preferred_element_type=jnp.float32)
            sbuf[panel, :, cols] = jnp.dot(
                dbuf[panel], pivot, precision=lax.Precision.HIGHEST,
                preferred_element_type=jnp.float32).astype(jnp.bfloat16)
            return 0

        lax.fori_loop(0, columns // TILE, columns_of, 0)

    def spread(panel, step):
        return pltpu.make_async_remote_copy(
            src_ref=sbuf.at[panel], dst_ref=sbuf.at[panel],
            send_sem=ssend_sem.at[panel, step], recv_sem=srecv_sem.at[panel],
            device_id={"aux": lax.rem(a + step, aux)}, device_id_type=MESH)

    def settle(panel):
        solve(panel)
        for step in range(1, aux):
            spread(panel, step).start()

    before_last = max(mains - 2, cut_at)

    def update(j, _):
        at = jnp.where(jnp.logical_or(j < cut_at, j == mains - 1), j, j + 1)
        at = jnp.where(j == before_last, cut_at, at)

        def tile(i, _):
            here = pl.ds(pl.multiple_of(i * TILE, TILE), TILE)
            product = sum(
                lax.dot_general(
                    lbuf[:, panel, :, here].reshape(-1, TILE), sbuf[panel], CONTRACT,
                    preferred_element_type=jnp.float32)
                for panel in range(panels))
            mbuf[here] = (mbuf[here].astype(jnp.float32) - product).astype(jnp.bfloat16)
            return 0

        tiles = chunk // TILE
        lax.fori_loop(at * tiles, (at + 1) * tiles, tile, 0)
        return 0

    edges_in = cut_at + HOPS[2] + chips - 1
    last = max(pieces + chips, edges_in + 1)
    first = min(chips + panels + 1, last - 1 - (mains + 1) // 2)

    def done_by(t):
        if isinstance(t, int):
            ready = t - chips + 1
            if t < max(edges_in, before_last + chips):
                ready = min(t - chips, before_last)
            ready = mains if t == last - 1 else min(ready, 2 * (t - first + 1))
            return max(0, min(ready, mains))
        ready = jnp.where(t >= max(edges_in, before_last + chips), t - chips + 1,
                          jnp.minimum(t - chips, before_last))
        ready = jnp.minimum(ready, 2 * (t - first + 1))
        return jnp.clip(jnp.where(t == last - 1, mains, ready), 0, mains)

    def solves(t):
        for panel in range(panels):
            @pl.when(jnp.logical_and(t == (chips - 1 + panel if panel else 2), a == panel))
            def _(panel=panel):
                for before in range(panel):
                    spread(before, 1).wait_recv()
                settle(panel)

    def joins(t):
        @pl.when(t == 4)
        def _():
            rest_load.start()

        @pl.when(t == edges_in)
        def _():
            for zb in range(chips):
                swap(zb, edge_at, ("edge",), 1 - c).wait_recv()

        @pl.when(t == first)
        def _():
            rest_load.wait()
            for panel in range(panels):
                @pl.when(jnp.logical_and(a != panel, jnp.logical_or(a < panel, a >= panels)))
                def _(panel=panel):
                    spread(panel, 1).wait_recv()

    def tick(t, _):
        sized(t - WINDOW, own_sent)
        sized(t, own)
        sized(t - chips, complete)
        joins(t)
        lax.fori_loop(done_by(t - 1), done_by(t), update, 0)
        for step in range(1, chips):
            sized(t - WINDOW - step, functools.partial(passed, step))
            sized(t - step, functools.partial(pass_on, step))
        if not isinstance(t, int):
            hops(t)
            solves(t)
        return 0

    sized(0, own)
    body_load.wait()
    tail_load.wait()
    pack(ebuf, ltail, me)
    sized(1, own)

    for block in range(panels):
        @pl.when(a == block)
        def _(block=block):
            shape = (lbuf.shape[0], panels - block, lbuf.shape[2], width)
            lbuf[:, pl.ds(block, panels - block), :, pl.ds(0, width)] = jnp.zeros(shape, jnp.bfloat16)

    for step in range(1, chips):
        sized(1 - step, functools.partial(pass_on, step))
    pivot_load.wait()
    inverse_load.wait()
    steady = max(last - ENDING, cut_at + HOPS[2] + chips - 1, chips + panels, first + 1)
    steady = min(steady, last)
    lax.fori_loop(2, steady, tick, 0)
    for t in range(steady, last):
        tick(t, 0)

    for t in range(last, last + WINDOW):
        sized(t - WINDOW, own_sent)
        for step in range(1, chips):
            sized(t - WINDOW - step, functools.partial(passed, step))
    hops_sent()
    for panel in range(panels):
        @pl.when(a == panel)
        def _(panel=panel):
            for step in range(1, aux):
                spread(panel, step).wait_send()


def write_kernel(chunk, mbuf, sbuf, ltail, out_hbm, solved_hbm, tbuf, out_sem, tail_sem, s_sem):
    rows = mbuf.shape[0]
    panels, width = sbuf.shape[:2]
    pair = ltail.shape[0]
    mains = out_sem.shape[0]
    whole = mains * chunk

    def main(j):
        here = pl.ds(pl.multiple_of(j * chunk, chunk), chunk)
        return pltpu.make_async_copy(mbuf.at[here], out_hbm.at[here], out_sem.at[j])

    lax.fori_loop(0, mains, lambda j, _: (main(j).start(), 0)[1], 0)
    solved = pltpu.make_async_copy(sbuf, solved_hbm, s_sem)
    solved.start()

    left = rows - whole
    part = width // pair
    groups = panels * part // SUBLANES
    tiles, ragged, fit = packing(left, groups)

    stored = []

    def written(k):
        at, size = stored[k]
        return pltpu.make_async_copy(
            tbuf.at[pl.ds(at, size)], out_hbm.at[pl.ds(whole + at, size)], tail_sem.at[k])

    def store(at, total):
        size = total.shape[0]
        held = mbuf[pl.ds(whole + at, size)].astype(jnp.float32)
        tbuf[pl.ds(at, size)] = (held - total).astype(jnp.bfloat16)
        stored.append((at, size))
        if len(stored) > 1:
            written(len(stored) - 2).start()

    def lanes_of(panel, i):
        return ltail[:, pl.ds((i * panels + panel) * part, part)].reshape(width, LANES)

    for i in range(0, tiles, TILE // LANES):
        both = range(i, min(tiles, i + TILE // LANES))
        store(i * LANES, sum(
            lax.dot_general(
                jnp.concatenate([lanes_of(panel, i) for i in both], axis=1), sbuf[panel], CONTRACT,
                preferred_element_type=jnp.float32)
            for panel in range(panels)))
    if ragged:
        base = panels * tiles * part
        total = 0.0
        for g in range(groups):
            slot, off = g // fit, g % fit * ragged
            panel, at = g * SUBLANES // part, g * SUBLANES % part
            packed = ltail[:, pl.ds(base + slot * SUBLANES, SUBLANES)].reshape(-1, LANES)
            solved_rows = sbuf[panel].reshape(pair, part, -1)[:, at:at + SUBLANES]
            total = total + lax.dot_general(
                packed, solved_rows.reshape(pair * SUBLANES, -1), CONTRACT,
                preferred_element_type=jnp.float32)[off:off + ragged]
        store(tiles * LANES, total)
    early = mains // 2
    lax.fori_loop(0, early, lambda j, _: (main(j).wait(), 0)[1], 0)
    written(len(stored) - 1).start()
    lax.fori_loop(early, mains, lambda j, _: (main(j).wait(), 0)[1], 0)
    solved.wait()
    for k in range(len(stored)):
        written(k).wait()


def shards(aux, pair, m_panels, lower_cols, diag_inverses):
    panels, width = diag_inverses.shape[:2]
    rows, columns = m_panels.shape
    part = lower_cols.shape[1]
    chips = pair // CORES
    chunk = max(CHUNK, (width // TILE + 1) * TILE)
    mains = (rows - 1) // chunk - LATE
    left = rows - mains * chunk
    pieces = mains + len(late_pieces(chunk, panels, part, left))
    cut_at = min(CUT, mains - 1)
    detours = min(panels, aux - panels) if chips >= 4 else 0
    anywhere = pl.BlockSpec(memory_space=pl.ANY)
    vmem = pl.BlockSpec(memory_space=pltpu.VMEM)
    dma = pltpu.SemaphoreType.DMA
    held, solved, ltail = pl.pallas_call(
        functools.partial(gather_kernel, aux, chips, chunk, cut_at),
        in_specs=[anywhere, anywhere, anywhere],
        out_specs=[vmem, vmem, vmem],
        out_shape=[
            pltpu.VMEM((rows, columns), jnp.bfloat16),
            pltpu.VMEM((panels, width, columns), jnp.bfloat16),
            pltpu.VMEM((pair, tail_rows(panels, part, left), LANES), jnp.bfloat16),
        ],
        scratch_shapes=[
            pltpu.VMEM((pair, panels, part, mains * chunk), jnp.bfloat16),
            pltpu.VMEM((panels, part, left), jnp.bfloat16),
            pltpu.VMEM((panels, width, width), jnp.float32),
            pltpu.VMEM((detours, chips, panels, part, LANES), jnp.bfloat16),
            dma((6,)),
            dma((chips, pieces + 2)),
            dma((chips, pieces + 2)),
            dma((chips, pieces + 2)),
            dma((chips, pieces + 2)),
            dma((chips, pieces + 2)),
            dma((panels,)),
            dma((panels, aux)),
            dma((2, max(detours, 1), chips)),
            dma((max(detours, 1), chips)),
        ],
        compiler_params=pltpu.CompilerParams(
            collective_id=0, has_side_effects=True, vmem_limit_bytes=36 * 1024 * 1024),
    )(m_panels, lower_cols, diag_inverses)
    return pl.pallas_call(
        functools.partial(write_kernel, chunk),
        in_specs=[vmem, vmem, vmem],
        out_specs=[anywhere, anywhere],
        out_shape=[
            jax.ShapeDtypeStruct((rows, columns), jnp.bfloat16),
            jax.ShapeDtypeStruct((panels, width, columns), jnp.bfloat16),
        ],
        scratch_shapes=[
            pltpu.VMEM((left, columns), jnp.bfloat16),
            dma((mains,)),
            dma((left // TILE + 2,)),
            dma,
        ],
        compiler_params=pltpu.CompilerParams(vmem_limit_bytes=8 * 1024 * 1024),
    )(held, solved, ltail)


def solution(mesh):
    placed = (P("aux", "pair"), P(None, "pair", "aux"), P())
    return jax.shard_map(
        functools.partial(shards, mesh.shape["aux"], mesh.shape["pair"]),
        mesh=mesh,
        in_specs=placed,
        out_specs=(P("aux", "pair"), P(None, None, "pair")),
        check_vma=False,
    )
```

```python
import functools

import jax
import jax.numpy as jnp
from jax import lax
from jax.experimental import pallas as pl
from jax.experimental.pallas import tpu as pltpu
from jax.sharding import PartitionSpec as P

CHUNK = 1024
LATE = 1
TILE = 256
LANES = 128
SUBLANES = 16
CORES = 2
CUT = 1
HOPS = (2, 5, 6)
ENDING = 4
WINDOW = 2
CONTRACT = (((0,), (0,)), ((), ()))
MESH = pl.DeviceIdType.MESH


def packing(left, groups):
    ragged = left % LANES
    return left // LANES, ragged, LANES // ragged if ragged else groups


def tail_rows(panels, part, left):
    groups = panels * part // SUBLANES
    tiles, ragged, fit = packing(left, groups)
    return panels * tiles * part + (-(-groups // fit) * SUBLANES if ragged else 0)


def late_pieces(chunk, panels, part, left):
    tiles = left // LANES
    cuts = {0, max(0, tiles - TILE // LANES)}
    for k in range(1, LATE + 1):
        cuts.add(min(k * (chunk // LANES), tiles))
    cuts = sorted(cuts)
    starts = [cut * panels * part for cut in cuts]
    ends = starts[1:] + [tail_rows(panels, part, left)]
    return [(start, end - start) for start, end in zip(starts, ends) if end > start]


def pack(ebuf, ltail, me):
    panels, part, left = ebuf.shape
    groups = panels * part // SUBLANES
    tiles, ragged, fit = packing(left, groups)
    for panel in range(panels):
        for i in range(tiles):
            at = (i * panels + panel) * part
            ltail[me, pl.ds(at, part)] = ebuf[panel, :, pl.ds(i * LANES, LANES)]
    if not ragged:
        return
    base = panels * tiles * part
    end = ebuf[:, :, pl.ds(tiles * LANES, ragged)].reshape(groups, SUBLANES, ragged)
    row = lax.broadcasted_iota(jnp.int32, (ragged, LANES), 0)
    lane = lax.broadcasted_iota(jnp.int32, (ragged, LANES), 1)
    for slot in range(-(-groups // fit)):
        total = jnp.zeros((SUBLANES, LANES), jnp.float32)
        for g in range(slot * fit, min(groups, (slot + 1) * fit)):
            place = (lane == row + (g - slot * fit) * ragged).astype(jnp.bfloat16)
            total = total + jnp.dot(end[g], place, preferred_element_type=jnp.float32)
        ltail[me, pl.ds(base + slot * SUBLANES, SUBLANES)] = total.astype(jnp.bfloat16)


def gather_kernel(aux, chips, chunk, cut_at, m_hbm, l_hbm, d_hbm, mbuf, sbuf, ltail,
                  lbuf, ebuf, dbuf, rbuf, load_sem, ring_sem, swap_sem, left_sem, right_sem, part_sem,
                  srecv_sem, ssend_sem, hop_sem, relay_sem):
    rows, columns = m_hbm.shape
    panels, width = d_hbm.shape[:2]
    whole = lbuf.shape[-1]
    mains = whole // chunk
    left = rows - whole
    late = late_pieces(chunk, panels, l_hbm.shape[1], left)
    pieces = mains + len(late)
    edge_at = pieces + 1
    detours = rbuf.shape[0]
    a = lax.axis_index("aux")
    me = lax.axis_index("pair")
    z, c = me // CORES, lax.rem(me, CORES)
    to_left = {"pair": lax.rem(z + chips - 1, chips) * CORES + c}
    to_right = {"pair": lax.rem(z + 1, chips) * CORES + c}
    partner = {"pair": z * CORES + 1 - c}

    def local(src, dst, i):
        return pltpu.make_async_copy(src, dst, load_sem.at[i])

    head_load = local(l_hbm.at[:, :, pl.ds(0, chunk)], lbuf.at[me, :, :, pl.ds(0, chunk)], 0)
    body_load = local(l_hbm.at[:, :, pl.ds(chunk, whole - chunk)],
                      lbuf.at[me, :, :, pl.ds(chunk, whole - chunk)], 1)
    tail_load = local(l_hbm.at[:, :, pl.ds(whole, left)], ebuf, 2)
    pivot_load = local(m_hbm.at[pl.ds(0, width)], mbuf.at[pl.ds(0, width)], 3)
    rest_load = local(m_hbm.at[pl.ds(width, rows - width)],
                      mbuf.at[pl.ds(width, rows - width)], 4)
    inverse_load = local(d_hbm, dbuf, 5)
    head_load.start()

    barrier = pltpu.get_barrier_semaphore()
    for peer in (to_left, to_right, partner):
        pl.semaphore_signal(barrier, inc=1, device_id=peer, device_id_type=MESH)
    for step in range(1, aux):
        peer = {"aux": lax.rem(a + step, aux)}
        pl.semaphore_signal(barrier, inc=1, device_id=peer, device_id_type=MESH)
    body_load.start()
    tail_load.start()
    pivot_load.start()
    inverse_load.start()
    pl.semaphore_wait(barrier, 2 + aux)
    head_load.wait()

    def piece(block, j, kind):
        name, *span = kind
        if name == "late":
            return ltail.at[block, pl.ds(*span)]
        if name == "head":
            return lbuf.at[block, pl.ds(0, *span), :, pl.ds(0, width)]
        if name == "bare":
            return lbuf.at[block, :, :, pl.ds(width, chunk - width)]
        if name == "edge":
            return lbuf.at[block, :, :, pl.ds((cut_at + 1) * chunk - LANES, LANES)]
        if name == "cut":
            return lbuf.at[block, :, :, pl.ds(cut_at * chunk, chunk - LANES)]
        at = j * chunk if isinstance(j, int) else pl.multiple_of(j * chunk, LANES)
        return lbuf.at[block, :, :, pl.ds(at, chunk)]

    def ring(zb, j, size, send, peer):
        ref = piece(zb * CORES + c, j, size)
        return pltpu.make_async_remote_copy(
            src_ref=ref, dst_ref=ref, send_sem=send.at[zb, j], recv_sem=ring_sem.at[zb, j],
            device_id=peer, device_id_type=MESH)

    def swap(zb, j, size, core):
        ref = piece(zb * CORES + core, j, size)
        return pltpu.make_async_remote_copy(
            src_ref=ref, dst_ref=ref, send_sem=part_sem.at[zb, j], recv_sem=swap_sem.at[zb, j],
            device_id=partner, device_id_type=MESH)

    def sized(j, act):
        if isinstance(j, int) and j > 0:
            if j == cut_at:
                act(edge_at, ("edge",))
                act(cut_at, ("cut",))
            elif j < mains:
                act(j, ("main",))
            elif j < pieces:
                act(j, ("late", *late[j - mains]))
            return
        if isinstance(j, int) and j < 0:
            return
        whole_piece = jnp.logical_or(j > 0, a >= panels)
        whole_piece = jnp.logical_and(whole_piece, jnp.logical_and(j >= 0, j < mains))
        whole_piece = jnp.logical_and(whole_piece, j != cut_at)

        @pl.when(whole_piece)
        def _():
            act(j, ("main",))

        for block in range(panels):
            @pl.when(jnp.logical_and(j == 0, a == block))
            def _(block=block):
                act(0, ("bare",))
                if block:
                    act(pieces, ("head", block))

        @pl.when(j == cut_at)
        def _():
            act(edge_at, ("edge",))
            act(cut_at, ("cut",))

        for k, span in enumerate(late):
            @pl.when(j == mains + k)
            def _(k=k, span=span):
                act(mains + k, ("late", *span))

    detoured = jnp.logical_and(a >= panels, a < panels + detours)
    lane = jnp.clip(a - panels, 0, max(detours - 1, 0))

    def via(zb, send):
        return pltpu.make_async_remote_copy(
            src_ref=piece(zb * CORES + c, edge_at, ("edge",)), dst_ref=rbuf.at[lane, zb],
            send_sem=send.at[zb, edge_at], recv_sem=hop_sem.at[0, lane, zb],
            device_id={"aux": 0}, device_id_type=MESH)

    def along(d, zb, peer):
        return pltpu.make_async_remote_copy(
            src_ref=rbuf.at[d, zb], dst_ref=rbuf.at[d, zb],
            send_sem=relay_sem.at[d, zb], recv_sem=hop_sem.at[1, d, zb],
            device_id=peer, device_id_type=MESH)

    def back(d, zb):
        return pltpu.make_async_remote_copy(
            src_ref=rbuf.at[d, zb], dst_ref=piece(zb * CORES + c, edge_at, ("edge",)),
            send_sem=relay_sem.at[d, zb], recv_sem=ring_sem.at[zb, edge_at],
            device_id={"aux": panels + d}, device_id_type=MESH)

    sides = ((0, 1, 1, to_left), (chips - 1, chips - 2, -1, to_right)) if detours else ()

    def hops(t):
        for end, near, sign, peer in sides:
            for d in range(detours):
                s = t - cut_at - HOPS[0]

                @pl.when(jnp.logical_and(a == 0, jnp.logical_and(
                    z == near, jnp.logical_and(s >= 0, s < chips - 1))))
                def _(s=s, d=d, near=near, sign=sign, peer=peer):
                    zb = near + sign * s
                    pltpu.make_async_remote_copy(
                        src_ref=rbuf.at[d, zb], dst_ref=rbuf.at[d, zb],
                        send_sem=relay_sem.at[d, zb], recv_sem=hop_sem.at[0, d, zb],
                        device_id=peer, device_id_type=MESH).wait_recv()
                    along(d, zb, peer).start()

                s = t - cut_at - HOPS[1]

                @pl.when(jnp.logical_and(a == 0, jnp.logical_and(
                    z == end, jnp.logical_and(s >= 0, s < chips - 1))))
                def _(s=s, d=d, near=near, sign=sign, peer=peer):
                    zb = near + sign * s
                    along(d, zb, peer).wait_recv()
                    back(d, zb).start()

            s = t - cut_at - HOPS[2]

            @pl.when(jnp.logical_and(detoured, jnp.logical_and(
                z == end, jnp.logical_and(s >= 0, s < chips - 1))))
            def _(s=s, near=near, sign=sign, peer=peer):
                zb = near + sign * s
                ring(zb, edge_at, ("edge",), left_sem, peer).wait_recv()
                swap(zb, edge_at, ("edge",), c).start()

    def hops_sent():
        for end, near, sign, peer in sides:
            def relayed(s, _, end=end, near=near, sign=sign, peer=peer):
                zb = near + sign * s
                for d in range(detours):
                    @pl.when(jnp.logical_and(a == 0, z == near))
                    def _(d=d):
                        along(d, zb, peer).wait_send()

                    @pl.when(jnp.logical_and(a == 0, z == end))
                    def _(d=d):
                        back(d, zb).wait_send()

                @pl.when(jnp.logical_and(detoured, z == end))
                def _():
                    swap(zb, edge_at, ("edge",), c).wait_send()
                return 0

            lax.fori_loop(0, chips - 1, relayed, 0)

    def leave(zb, j, size, leftward, rightward, act):
        goes_left = jnp.logical_and(leftward, z > 0)
        goes_right = jnp.logical_and(rightward, z < chips - 1)
        if size[0] == "edge" and detours:
            round_left = jnp.logical_and(goes_left, jnp.logical_and(detoured, z == 1))
            round_right = jnp.logical_and(goes_right, jnp.logical_and(detoured, z == chips - 2))
            goes_left = jnp.logical_and(goes_left, jnp.logical_not(round_left))
            goes_right = jnp.logical_and(goes_right, jnp.logical_not(round_right))

            @pl.when(round_left)
            def _():
                act(via(zb, left_sem))

            @pl.when(round_right)
            def _():
                act(via(zb, right_sem))

        @pl.when(goes_left)
        def _():
            act(ring(zb, j, size, left_sem, to_left))

        @pl.when(goes_right)
        def _():
            act(ring(zb, j, size, right_sem, to_right))

        act(swap(zb, j, size, c))

    def send(zb, j, size, leftward, rightward):
        leave(zb, j, size, leftward, rightward, lambda copy: copy.start())

    def sent(zb, j, size, leftward, rightward):
        leave(zb, j, size, leftward, rightward, lambda copy: copy.wait_send())

    def arrives(zb, size, end):
        here = jnp.logical_and(zb >= 0, zb < chips)
        if size[0] == "edge" and detours:
            here = jnp.logical_and(here, jnp.logical_not(jnp.logical_and(detoured, z == end)))
        return here

    def own(j, size):
        send(z, j, size, True, True)

    def own_sent(j, size):
        sent(z, j, size, True, True)

    def pass_on(step, j, size):
        @pl.when(arrives(z + step, size, 0))
        def _():
            ring(z + step, j, size, left_sem, to_left).wait_recv()
            send(z + step, j, size, True, False)

        @pl.when(arrives(z - step, size, chips - 1))
        def _():
            ring(z - step, j, size, right_sem, to_right).wait_recv()
            send(z - step, j, size, False, True)

    def passed(step, j, size):
        @pl.when(arrives(z + step, size, 0))
        def _():
            sent(z + step, j, size, True, False)

        @pl.when(arrives(z - step, size, chips - 1))
        def _():
            sent(z - step, j, size, False, True)

    def complete(j, size):
        if size[0] == "edge":
            return
        for zb in range(chips):
            swap(zb, j, size, 1 - c).wait_recv()

    def solve(panel):
        def columns_of(i, _):
            cols = pl.ds(pl.multiple_of(i * TILE, TILE), TILE)
            pivot = mbuf[pl.ds(0, width), cols].astype(jnp.float32)
            for before in range(panel):
                factor = lbuf[:, before, :, pl.ds(0, width)].reshape(-1, width)
                pivot = pivot - lax.dot_general(
                    factor, sbuf[before, :, cols], CONTRACT, preferred_element_type=jnp.float32)
            sbuf[panel, :, cols] = jnp.dot(
                dbuf[panel], pivot, precision=lax.Precision.HIGHEST,
                preferred_element_type=jnp.float32).astype(jnp.bfloat16)
            return 0

        lax.fori_loop(0, columns // TILE, columns_of, 0)

    def spread(panel, step):
        return pltpu.make_async_remote_copy(
            src_ref=sbuf.at[panel], dst_ref=sbuf.at[panel],
            send_sem=ssend_sem.at[panel, step], recv_sem=srecv_sem.at[panel],
            device_id={"aux": lax.rem(a + step, aux)}, device_id_type=MESH)

    def settle(panel):
        solve(panel)
        for step in range(1, aux):
            spread(panel, step).start()

    before_last = max(mains - 2, cut_at)

    def update(j, _):
        at = jnp.where(jnp.logical_or(j < cut_at, j == mains - 1), j, j + 1)
        at = jnp.where(j == before_last, cut_at, at)

        def tile(i, _):
            here = pl.ds(pl.multiple_of(i * TILE, TILE), TILE)
            product = sum(
                lax.dot_general(
                    lbuf[:, panel, :, here].reshape(-1, TILE), sbuf[panel], CONTRACT,
                    preferred_element_type=jnp.float32)
                for panel in range(panels))
            mbuf[here] = (mbuf[here].astype(jnp.float32) - product).astype(jnp.bfloat16)
            return 0

        tiles = chunk // TILE
        lax.fori_loop(at * tiles, (at + 1) * tiles, tile, 0)
        return 0

    edges_in = cut_at + HOPS[2] + chips - 1
    last = max(pieces + chips, edges_in + 1)
    first = min(chips + panels + 1, last - 1 - (mains + 1) // 2)

    def done_by(t):
        if isinstance(t, int):
            ready = t - chips + 1
            if t < max(edges_in, before_last + chips):
                ready = min(t - chips, before_last)
            ready = mains if t == last - 1 else min(ready, 2 * (t - first + 1))
            return max(0, min(ready, mains))
        ready = jnp.where(t >= max(edges_in, before_last + chips), t - chips + 1,
                          jnp.minimum(t - chips, before_last))
        ready = jnp.minimum(ready, 2 * (t - first + 1))
        return jnp.clip(jnp.where(t == last - 1, mains, ready), 0, mains)

    def solves(t):
        for panel in range(panels):
            @pl.when(jnp.logical_and(t == (chips - 1 + panel if panel else 2), a == panel))
            def _(panel=panel):
                for before in range(panel):
                    spread(before, 1).wait_recv()
                settle(panel)

    def joins(t):
        @pl.when(t == 4)
        def _():
            rest_load.start()

        @pl.when(t == edges_in)
        def _():
            for zb in range(chips):
                swap(zb, edge_at, ("edge",), 1 - c).wait_recv()

        @pl.when(t == first)
        def _():
            rest_load.wait()
            for panel in range(panels):
                @pl.when(jnp.logical_and(a != panel, jnp.logical_or(a < panel, a >= panels)))
                def _(panel=panel):
                    spread(panel, 1).wait_recv()

    def tick(t, _):
        sized(t - WINDOW, own_sent)
        sized(t, own)
        sized(t - chips, complete)
        joins(t)
        lax.fori_loop(done_by(t - 1), done_by(t), update, 0)
        for step in range(1, chips):
            sized(t - WINDOW - step, functools.partial(passed, step))
            sized(t - step, functools.partial(pass_on, step))
        if not isinstance(t, int):
            hops(t)
            solves(t)
        return 0

    sized(0, own)
    body_load.wait()
    tail_load.wait()
    pack(ebuf, ltail, me)
    sized(1, own)

    for block in range(panels):
        @pl.when(a == block)
        def _(block=block):
            shape = (lbuf.shape[0], panels - block, lbuf.shape[2], width)
            lbuf[:, pl.ds(block, panels - block), :, pl.ds(0, width)] = jnp.zeros(shape, jnp.bfloat16)

    for step in range(1, chips):
        sized(1 - step, functools.partial(pass_on, step))
    pivot_load.wait()
    inverse_load.wait()
    steady = max(last - ENDING, cut_at + HOPS[2] + chips - 1, chips + panels, first + 1)
    steady = min(steady, last)
    lax.fori_loop(2, steady, tick, 0)
    for t in range(steady, last):
        tick(t, 0)

    for t in range(last, last + WINDOW):
        sized(t - WINDOW, own_sent)
        for step in range(1, chips):
            sized(t - WINDOW - step, functools.partial(passed, step))
    hops_sent()
    for panel in range(panels):
        @pl.when(a == panel)
        def _(panel=panel):
            for step in range(1, aux):
                spread(panel, step).wait_send()


def write_kernel(chunk, mbuf, sbuf, ltail, out_hbm, solved_hbm, tbuf, out_sem, tail_sem, s_sem):
    rows = mbuf.shape[0]
    panels, width = sbuf.shape[:2]
    pair = ltail.shape[0]
    mains = out_sem.shape[0]
    whole = mains * chunk

    def main(j):
        here = pl.ds(j * chunk, chunk)
        return pltpu.make_async_copy(mbuf.at[here], out_hbm.at[here], out_sem.at[j])

    for j in range(mains):
        main(j).start(priority=j % 2)
    solved = pltpu.make_async_copy(sbuf, solved_hbm, s_sem)
    solved.start()

    left = rows - whole
    part = width // pair
    groups = panels * part // SUBLANES
    tiles, ragged, fit = packing(left, groups)

    stored = []

    def written(k):
        at, size = stored[k]
        return pltpu.make_async_copy(
            tbuf.at[pl.ds(at, size)], out_hbm.at[pl.ds(whole + at, size)], tail_sem.at[k])

    def store(at, total):
        size = total.shape[0]
        held = mbuf[pl.ds(whole + at, size)].astype(jnp.float32)
        tbuf[pl.ds(at, size)] = (held - total).astype(jnp.bfloat16)
        stored.append((at, size))
        if len(stored) > 1:
            written(len(stored) - 2).start()

    def lanes_of(panel, i):
        return ltail[:, pl.ds((i * panels + panel) * part, part)].reshape(width, LANES)

    for i in range(0, tiles, TILE // LANES):
        both = range(i, min(tiles, i + TILE // LANES))
        store(i * LANES, sum(
            lax.dot_general(
                jnp.concatenate([lanes_of(panel, i) for i in both], axis=1), sbuf[panel], CONTRACT,
                preferred_element_type=jnp.float32)
            for panel in range(panels)))
    if ragged:
        base = panels * tiles * part
        total = 0.0
        for g in range(groups):
            slot, off = g // fit, g % fit * ragged
            panel, at = g * SUBLANES // part, g * SUBLANES % part
            packed = ltail[:, pl.ds(base + slot * SUBLANES, SUBLANES)].reshape(-1, LANES)
            solved_rows = sbuf[panel].reshape(pair, part, -1)[:, at:at + SUBLANES]
            total = total + lax.dot_general(
                packed, solved_rows.reshape(pair * SUBLANES, -1), CONTRACT,
                preferred_element_type=jnp.float32)[off:off + ragged]
        store(tiles * LANES, total)
    early = mains // 2
    lax.fori_loop(0, early, lambda j, _: (main(j).wait(), 0)[1], 0)
    written(len(stored) - 1).start()
    lax.fori_loop(early, mains, lambda j, _: (main(j).wait(), 0)[1], 0)
    solved.wait()
    for k in range(len(stored)):
        written(k).wait()


def shards(aux, pair, m_panels, lower_cols, diag_inverses):
    panels, width = diag_inverses.shape[:2]
    rows, columns = m_panels.shape
    part = lower_cols.shape[1]
    chips = pair // CORES
    chunk = max(CHUNK, (width // TILE + 1) * TILE)
    mains = (rows - 1) // chunk - LATE
    left = rows - mains * chunk
    pieces = mains + len(late_pieces(chunk, panels, part, left))
    cut_at = min(CUT, mains - 1)
    detours = min(panels, aux - panels) if chips >= 4 else 0
    anywhere = pl.BlockSpec(memory_space=pl.ANY)
    vmem = pl.BlockSpec(memory_space=pltpu.VMEM)
    dma = pltpu.SemaphoreType.DMA
    held, solved, ltail = pl.pallas_call(
        functools.partial(gather_kernel, aux, chips, chunk, cut_at),
        in_specs=[anywhere, anywhere, anywhere],
        out_specs=[vmem, vmem, vmem],
        out_shape=[
            pltpu.VMEM((rows, columns), jnp.bfloat16),
            pltpu.VMEM((panels, width, columns), jnp.bfloat16),
            pltpu.VMEM((pair, tail_rows(panels, part, left), LANES), jnp.bfloat16),
        ],
        scratch_shapes=[
            pltpu.VMEM((pair, panels, part, mains * chunk), jnp.bfloat16),
            pltpu.VMEM((panels, part, left), jnp.bfloat16),
            pltpu.VMEM((panels, width, width), jnp.float32),
            pltpu.VMEM((detours, chips, panels, part, LANES), jnp.bfloat16),
            dma((6,)),
            dma((chips, pieces + 2)),
            dma((chips, pieces + 2)),
            dma((chips, pieces + 2)),
            dma((chips, pieces + 2)),
            dma((chips, pieces + 2)),
            dma((panels,)),
            dma((panels, aux)),
            dma((2, max(detours, 1), chips)),
            dma((max(detours, 1), chips)),
        ],
        compiler_params=pltpu.CompilerParams(
            collective_id=0, has_side_effects=True, vmem_limit_bytes=36 * 1024 * 1024),
    )(m_panels, lower_cols, diag_inverses)
    return pl.pallas_call(
        functools.partial(write_kernel, chunk),
        in_specs=[vmem, vmem, vmem],
        out_specs=[anywhere, anywhere],
        out_shape=[
            jax.ShapeDtypeStruct((rows, columns), jnp.bfloat16),
            jax.ShapeDtypeStruct((panels, width, columns), jnp.bfloat16),
        ],
        scratch_shapes=[
            pltpu.VMEM((left, columns), jnp.bfloat16),
            dma((mains,)),
            dma((left // TILE + 2,)),
            dma,
        ],
        compiler_params=pltpu.CompilerParams(vmem_limit_bytes=8 * 1024 * 1024),
    )(held, solved, ltail)


def solution(mesh):
    placed = (P("aux", "pair"), P(None, "pair", "aux"), P())
    return jax.shard_map(
        functools.partial(shards, mesh.shape["aux"], mesh.shape["pair"]),
        mesh=mesh,
        in_specs=placed,
        out_specs=(P("aux", "pair"), P(None, None, "pair")),
        check_vma=False,
    )
```
